32 devices in a mesh: row: 8 (over z, x), col: 4 (over y, core).
Axes of the slice: x: 2, y: 2, z: 4, core: 2. Of those that a mesh axis runs over, the one named last changes fastest.
Arguments:
- object_field: float32 [2, 2, 4096, 2048], P(None, None, 'row', 'col'), may hold values from -5 to 5
- probe_field: float32 [2, 256, 256], replicated, may hold values from -6 to 6
- propagator_phase: float32 [256, 256], replicated, may hold values from -3.140625 to 3.140625
- positions: int32 [8, 4, 4, 2], P('row', 'col'), may hold values from 0 to 511
- counts: int32 [8, 4], P('row', 'col'), may hold values from 2 to 4, as said below
- amplitudes: bfloat16 [8, 4, 4, 256, 256], P('row', 'col'), may hold values from 0.19921875 to 2.5
Outputs:
- object_gradient: float32 [2, 2, 4096, 2048], P(None, None, 'row', 'col')
The draws below stay inside these ranges and needn't reach their ends.
Inputs may be any that keep to these rules, and one draw needn't show every extreme that they name: `counts`: each tile holds from 2 to 4 live slots; in every draw some tile holds 4 and some tile holds 2.
All inputs are finite; a program needn't handle non-finite values.
Results may differ from the reference program's by a relative error of at most 0.018.
Values sent between devices are 32-bit elements; how exact they have to be, the bound alone decides.
No kernel may reach another device: no remote copies, remote signals or barrier semaphores. Data moves between devices by JAX's collectives and lax.ppermute only.
A program may use at most 128 MiB of HBM per device.

```python
import math
import jax
import jax.numpy as jnp
from jax import lax

N = 256
TILE = 512
MAXP = 4
SLICES = 2
HEIGHT = 4096
WIDTH = 2048
N_ROW = 8
N_COL = 4


def draw_counts(key, part):
    key_base, key_high, key_step = jax.random.split(jax.random.fold_in(key, 17), 3)
    tiles_all = N_ROW * N_COL
    base_counts = jax.random.randint(key_base, (tiles_all,), MAXP // 2, MAXP + 1, dtype=jnp.int32)
    high_spot = jax.random.randint(key_high, (), 0, tiles_all, dtype=jnp.int32)
    low_spot = (high_spot + 1 + jax.random.randint(key_step, (), 0, tiles_all - 1, dtype=jnp.int32)) % tiles_all
    base_counts = base_counts.at[high_spot].set(MAXP).at[low_spot].set(MAXP // 2)
    return base_counts.reshape(N_ROW, N_COL).astype(jnp.int32)


def plant(values, key, smallest, high):
    shape = values.shape
    place = [jax.random.randint(jax.random.fold_in(key, axis), (), 0, shape[axis]) for axis in range(len(shape))]
    values = values.at[tuple(place)].set(smallest)
    longest = shape.index(max(shape))
    place[longest] = (place[longest] + 1) % shape[longest]
    return values.at[tuple(place)].set(high)


def levels(rng, shape, cuts, smallest, top_value):
    factor_of = 1.0
    for position, shards_of in cuts:
        draws = jax.random.uniform(jax.random.fold_in(jax.random.fold_in(rng, 6), position), (shards_of,), jnp.float32, smallest / len(cuts), top_value / len(cuts))
        factor_of = factor_of * jnp.repeat(jnp.exp(draws), shape[position] // shards_of).reshape((-1,) + (1,) * (len(shape) - 1 - position))
    return factor_of


def normal_values(rng, shape, scale, bound, cuts=(), held_as=jnp.bfloat16):
    entries = scale * jax.random.normal(rng, shape, jnp.float32)
    if cuts:
        entries = entries * levels(rng, shape, cuts, -0.22, 0.18)
    return jnp.clip(entries, -bound, bound).astype(held_as)


def setup_inputs(seed: int = 0) -> dict:
    streams_of = jax.random.split(jax.random.key(seed), 7)
    return {
        "object_field": normal_values(streams_of[0], (SLICES, 2, HEIGHT, WIDTH), 0.7, 5.0, ((2, 8), (3, 4)), jnp.float32),
        "probe_field": normal_values(streams_of[1], (2, N, N), 1.0, 6.0, (), jnp.float32),
        "propagator_phase": jnp.clip(jax.random.uniform(streams_of[2], (N, N), jnp.float32, -3.140625, 3.140625), -3.140625, 3.140625),
        "positions": plant(jax.random.randint(streams_of[3], (N_ROW, N_COL, MAXP, 2), 0, TILE), jax.random.fold_in(streams_of[3], 1), 0, TILE - 1).astype(jnp.int32),
        "counts": draw_counts(jax.random.fold_in(streams_of[6], 71), 0),
        "amplitudes": jnp.clip(jnp.exp(math.log(2.5) - 2.5296425 * jax.random.uniform(streams_of[5], (N_ROW, N_COL, MAXP, N, N), jnp.float32) ** levels(streams_of[5], (N_ROW, N_COL, MAXP, N, N), ((0, 8), (1, 4)), -0.2, 0.2)), 0.19921875, 2.5).astype(jnp.bfloat16),
    }


floor_value = 0.1

def dft_tables(length, sign):
    indices = jnp.arange(length, dtype=jnp.int32)
    turns = indices[:, None] * indices[None, :] % length
    angles = turns.astype(jnp.float32) * (2.0 * math.pi / length)
    cosine = jnp.cos(angles) / math.sqrt(length)
    sine = sign * jnp.sin(angles) / math.sqrt(length)
    left_table = jnp.concatenate([jnp.concatenate([cosine, sine], 1), jnp.concatenate([-sine, cosine], 1)], 0)
    right_table = jnp.concatenate([jnp.concatenate([cosine, -sine], 1), jnp.concatenate([sine, cosine], 1)], 0)
    return (left_table.astype(jnp.bfloat16), right_table.astype(jnp.bfloat16))

def transform(field, sign):
    batched = field.shape[0]
    length = field.shape[-1]
    left_table, right_table = dft_tables(length, sign)
    stacked = field.astype(jnp.bfloat16).reshape(batched, 2 * length, length)
    middle = jnp.einsum('ij,bjk->bik', left_table.astype(jnp.float32), stacked.astype(jnp.float32), precision=lax.Precision.HIGHEST)
    middle = middle.reshape(batched, 2, length, length).transpose(0, 2, 1, 3).reshape(batched, length, 2 * length).astype(jnp.bfloat16)
    result = jnp.einsum('bik,kj->bij', middle.astype(jnp.float32), right_table.astype(jnp.float32), precision=lax.Precision.HIGHEST)
    return result.reshape(batched, length, 2, length).transpose(0, 2, 1, 3)

def product_of(left_wave, right_wave):
    left_real, left_imag = (left_wave[..., 0, :, :], left_wave[..., 1, :, :])
    right_real, right_imag = (right_wave[..., 0, :, :], right_wave[..., 1, :, :])
    return jnp.stack([left_real * right_real - left_imag * right_imag, left_real * right_imag + left_imag * right_real], -3)

def conj_product(left_wave, right_wave):
    left_real, left_imag = (left_wave[..., 0, :, :], left_wave[..., 1, :, :])
    right_real, right_imag = (right_wave[..., 0, :, :], right_wave[..., 1, :, :])
    return jnp.stack([left_real * right_real + left_imag * right_imag, left_imag * right_real - left_real * right_imag], -3)

def slot_gradients(patches, probe_field, propagator, measured, valid):
    first_slice = patches[:, 0]
    second_slice = patches[:, 1]
    lit_wave = product_of(probe_field, first_slice)
    spread_wave = transform(product_of(propagator, transform(lit_wave, 1.0)), -1.0)
    exit_wave = product_of(spread_wave, second_slice)
    far_field = transform(exit_wave, 1.0)
    magnitude = jnp.sqrt(far_field[:, 0] ** 2 + far_field[:, 1] ** 2)
    ratio = 1.0 - measured / jnp.maximum(magnitude, floor_value)
    residual_far = far_field * ratio[:, None]
    back_wave = transform(residual_far, -1.0)
    grad_second = conj_product(back_wave, spread_wave)
    inner_wave = conj_product(back_wave, second_slice)
    first_wave = transform(conj_product(transform(inner_wave, 1.0), propagator), -1.0)
    grad_first = conj_product(first_wave, probe_field)
    return jnp.stack([grad_first, grad_second], 1) * valid[:, None, None, None, None]

def run_batch(gradient, window, probe_field, propagator, slot_places, measured, probe_count, start_slot, per_batch):
    length = probe_field.shape[-1]
    anchor = jnp.int32(0)
    places = slot_places[start_slot:start_slot + per_batch]
    patches = jax.vmap(lambda slot_place: lax.dynamic_slice(window, (anchor, anchor, slot_place[0], slot_place[1]), (2, 2, length, length)))(places)
    valid = (start_slot + jnp.arange(per_batch, dtype=jnp.int32) < probe_count).astype(jnp.float32)
    grads = slot_gradients(patches, probe_field, propagator, measured[start_slot:start_slot + per_batch].astype(jnp.float32), valid)
    for member in range(per_batch):
        corner_at = (anchor, anchor, places[member, 0], places[member, 1])
        current = lax.dynamic_slice(gradient, corner_at, (2, 2, length, length))
        gradient = lax.dynamic_update_slice(gradient, current + grads[member], corner_at)
    return gradient

def tile_gradient(window, probe_field, propagator_phase, slot_places, probe_count, measured):
    per_batch = slot_places.shape[0] // 2
    propagator = jnp.stack([jnp.cos(propagator_phase), jnp.sin(propagator_phase)], 0)
    gradient = jnp.zeros(window.shape, jnp.float32)
    gradient = run_batch(gradient, window, probe_field, propagator, slot_places, measured, probe_count, 0, per_batch)
    gradient = run_batch(gradient, window, probe_field, propagator, slot_places, measured, probe_count, per_batch, per_batch)
    return gradient

def reference(object_field, probe_field, propagator_phase, positions, counts, amplitudes):
    height = object_field.shape[2]
    width = object_field.shape[3]
    extended = jnp.concatenate([object_field, object_field[:, :, :N, :]], 2)
    extended = jnp.concatenate([extended, extended[:, :, :, :N]], 3)
    anchor = jnp.int32(0)

    def visit(device_index, gradient_sum):
        device_index = jnp.asarray(device_index).astype(jnp.int32)
        row_index = device_index // N_COL
        col_index = device_index % N_COL
        row_start = (row_index * TILE).astype(jnp.int32)
        col_start = (col_index * TILE).astype(jnp.int32)
        corner_at = (anchor, anchor, row_start, col_start)
        window = lax.dynamic_slice(extended, corner_at, (SLICES, 2, TILE + N, TILE + N))
        local = tile_gradient(window, probe_field, propagator_phase, positions[row_index, col_index], counts[row_index, col_index], amplitudes[row_index, col_index])
        current = lax.dynamic_slice(gradient_sum, corner_at, (SLICES, 2, TILE + N, TILE + N))
        return lax.dynamic_update_slice(gradient_sum, current + local, corner_at)
    gradient_sum = lax.fori_loop(0, N_ROW * N_COL, visit, jnp.zeros((SLICES, 2, height + N, width + N), jnp.float32))
    folded = gradient_sum[:, :, :height, :width]
    folded = folded.at[:, :, :N, :].add(gradient_sum[:, :, height:, :width])
    folded = folded.at[:, :, :, :N].add(gradient_sum[:, :, :height, width:])
    folded = folded.at[:, :, :N, :N].add(gradient_sum[:, :, height:, width:])
    return folded
```

```python
import functools
import math

import jax
import jax.numpy as jnp
from jax import lax
from jax.experimental import pallas as pl
from jax.experimental.pallas import tpu as pltpu
from jax.sharding import PartitionSpec as P


floor_value = 0.1
lanes = 128


def shifted(block, axis, distance):
    devices = range(lax.axis_size(axis))
    route = [((i - distance) % len(devices), i) for i in devices]
    return lax.ppermute(block, axis, route)


def dft_tables(length):
    indices = jnp.arange(length, dtype=jnp.int32)
    turns = indices[:, None] * indices[None, :] % length
    angles = turns.astype(jnp.float32) * (2.0 * math.pi / length)
    cosine = jnp.cos(angles) / math.sqrt(length)
    sine = jnp.sin(angles) / math.sqrt(length)
    table_a = jnp.concatenate(
        [jnp.concatenate([cosine, sine], 1), jnp.concatenate([-sine, cosine], 1)], 0
    )
    table_b = jnp.concatenate(
        [jnp.concatenate([cosine, -sine], 1), jnp.concatenate([sine, cosine], 1)], 0
    )
    return (table_a.astype(jnp.bfloat16), table_b.astype(jnp.bfloat16))


def transform(wave, left_table, right_table):
    length = wave[0].shape[0]
    stacked = jnp.concatenate([part.astype(jnp.bfloat16) for part in wave], 0)
    middle = jnp.dot(left_table, stacked, preferred_element_type=jnp.float32)
    middle = middle.astype(jnp.bfloat16)
    middle = jnp.concatenate([middle[:length], middle[length:]], 1)
    result = jnp.dot(middle, right_table, preferred_element_type=jnp.float32)
    return result[:, :length], result[:, length:]


def product_of(left, right):
    return left[0] * right[0] - left[1] * right[1], left[0] * right[1] + left[1] * right[0]


def conj_product(left, right):
    return left[0] * right[0] + left[1] * right[1], left[1] * right[0] - left[0] * right[1]


def slots_kernel(
    places,
    count,
    object_ref,
    lower_ref,
    right_ref,
    corner_ref,
    probe_ref,
    propagator_ref,
    measured_ref,
    table_a_ref,
    table_b_ref,
    own_out,
    lower_out,
    right_out,
    corner_out,
    window,
    gradient,
    in_sems,
    out_sems,
):
    length = probe_ref.shape[-1]
    tile = object_ref.shape[-1]
    own_strips = tile // lanes
    halo_strips = length // lanes
    per_slot = halo_strips + 1

    def strip_copies(array, strips, row0, rows, sem, out):
        copies = []
        for plane in range(4):
            s, c = divmod(plane, 2)
            for k, strip in enumerate(strips):
                whole = array.at[s, c, :, pl.ds(k * lanes, lanes)]
                part = (gradient if out else window).at[s, c, strip, pl.ds(row0, rows), :]
                source, target = (part, whole) if out else (whole, part)
                copies.append(pltpu.make_async_copy(source, target, sem))
        return copies

    def all_copies(own, lower, right, corner, sems, out):
        own_range = range(own_strips)
        halo_range = range(own_strips, own_strips + halo_strips)
        return (
            strip_copies(lower, own_range, tile, length, sems.at[1], out)
            + strip_copies(corner, halo_range, tile, length, sems.at[3], out)
            + strip_copies(own, own_range, 0, tile, sems.at[0], out)
            + strip_copies(right, halo_range, 0, tile, sems.at[2], out)
        )

    loads = all_copies(object_ref, lower_ref, right_ref, corner_ref, in_sems, False)
    for copy in loads:
        copy.start()
    gradient[...] = jnp.zeros_like(gradient)
    for copy in loads:
        copy.wait()

    lane = lax.broadcasted_iota(jnp.int32, (length, lanes), 1)

    def fetch(s, row, strip, shift):
        out = []
        back = lax.rem(lanes - shift, lanes)
        for c in range(2):
            rolled = [
                pltpu.roll(window[s, c, strip + k, pl.ds(row, length), :], back, 1)
                for k in range(per_slot)
            ]
            out.append(
                jnp.concatenate(
                    [
                        jnp.where(lane < lanes - shift, rolled[k], rolled[k + 1])
                        for k in range(halo_strips)
                    ],
                    1,
                )
            )
        return tuple(out)

    def accumulate(s, row, strip, shift, wave):
        for c in range(2):
            rolled = [
                pltpu.roll(wave[c][:, k * lanes : (k + 1) * lanes], shift, 1)
                for k in range(halo_strips)
            ]
            for k in range(per_slot):
                if k == 0:
                    part = jnp.where(lane >= shift, rolled[0], 0.0)
                elif k == halo_strips:
                    part = jnp.where(lane < shift, rolled[k - 1], 0.0)
                else:
                    part = jnp.where(lane < shift, rolled[k - 1], rolled[k])
                spot = (s, c, strip + k, pl.ds(row, length), slice(None))
                gradient[spot] = gradient[spot] + part

    table_a = table_a_ref[...]
    table_b = table_b_ref[...]

    def one_slot(slot):
        row = places[2 * slot]
        column = places[2 * slot + 1]
        strip = column // lanes
        shift = lax.rem(column, lanes)
        probe = (probe_ref[0], probe_ref[1])
        propagator = (propagator_ref[0], propagator_ref[1])
        lit = product_of(probe, fetch(0, row, strip, shift))
        spread = transform(
            product_of(propagator, transform(lit, table_a, table_b)), table_b, table_a
        )
        second = fetch(1, row, strip, shift)
        far = transform(product_of(spread, second), table_a, table_b)
        power = far[0] * far[0] + far[1] * far[1]
        measured = measured_ref[slot].astype(jnp.float32)
        ratio = 1.0 - measured * jnp.minimum(lax.rsqrt(power), 1.0 / floor_value)
        back = transform((far[0] * ratio, far[1] * ratio), table_b, table_a)
        accumulate(1, row, strip, shift, conj_product(back, spread))
        inner = transform(conj_product(back, second), table_a, table_b)
        first = transform(conj_product(inner, propagator), table_b, table_a)
        accumulate(0, row, strip, shift, conj_product(first, probe))

    def body(slot, carry):
        one_slot(slot)
        return carry

    lax.fori_loop(0, count[0], body, 0)

    stores = all_copies(own_out, lower_out, right_out, corner_out, out_sems, True)
    for copy in stores:
        copy.start()
    for copy in stores:
        copy.wait()


def slot_pieces(places, count, own, lower, right, corner, probe, propagator, measured, tables):
    length = probe.shape[-1]
    tile = own.shape[-1]
    strips = (tile + length) // lanes
    whole = pl.BlockSpec(memory_space=pl.ANY)
    held = pl.BlockSpec(memory_space=pltpu.VMEM)
    scalar = pl.BlockSpec(memory_space=pltpu.SMEM)
    return pl.pallas_call(
        slots_kernel,
        name="slots",
        out_shape=[jax.ShapeDtypeStruct(x.shape, jnp.float32) for x in (own, lower, right, corner)],
        in_specs=[scalar, scalar] + [whole] * 4 + [held] * 5,
        out_specs=[whole] * 4,
        scratch_shapes=[
            pltpu.VMEM((2, 2, strips, tile + length, lanes), jnp.float32),
            pltpu.VMEM((2, 2, strips, tile + length, lanes), jnp.float32),
            pltpu.SemaphoreType.DMA((4,)),
            pltpu.SemaphoreType.DMA((4,)),
        ],
        compiler_params=pltpu.CompilerParams(vmem_limit_bytes=60 * 1024 * 1024),
    )(places, count, own, lower, right, corner, probe, propagator, measured, *tables)


def on_device(object_field, probe_field, propagator_phase, positions, counts, amplitudes):
    length = probe_field.shape[-1]
    tile_size = object_field.shape[-1]
    lower_near = shifted(object_field[:, :, :length, :length], "row", -1)
    lower_far = shifted(object_field[:, :, :length, length:], "row", -1)
    right = shifted(object_field[:, :, :, :length], "col", -1)
    corner = shifted(lower_near, "col", -1)
    lower = jnp.concatenate([lower_near, lower_far], 3)
    propagator = jnp.stack([jnp.cos(propagator_phase), jnp.sin(propagator_phase)], 0)
    own, lower, right, corner = slot_pieces(
        positions.reshape(-1),
        counts.reshape(-1),
        object_field,
        lower,
        right,
        corner,
        probe_field,
        propagator,
        amplitudes[0, 0],
        dft_tables(length),
    )
    corner = shifted(corner, "col", 1)
    lower_far = shifted(lower[:, :, :, length:], "row", 1)
    lower_near = shifted(lower[:, :, :, :length] + corner, "row", 1)
    right = shifted(right, "col", 1)
    gradient = own.at[:, :, :, :length].add(right)
    gradient = gradient.at[:, :, :length, length:].add(lower_far)
    gradient = gradient.at[:, :, :length, :length].add(lower_near)
    return gradient


def solution(mesh):
    return jax.shard_map(
        on_device,
        mesh=mesh,
        in_specs=(
            P(None, None, "row", "col"),
            P(),
            P(),
            P("row", "col", None, None),
            P("row", "col"),
            P("row", "col", None, None, None),
        ),
        out_specs=P(None, None, "row", "col"),
        check_vma=False,
    )
```

```python
import functools
import math

import jax
import jax.numpy as jnp
from jax import lax
from jax.experimental import pallas as pl
from jax.experimental.pallas import tpu as pltpu
from jax.sharding import PartitionSpec as P


floor_value = 0.1
lanes = 128


def shifted(block, axis, distance):
    devices = range(lax.axis_size(axis))
    route = [((i - distance) % len(devices), i) for i in devices]
    return lax.ppermute(block, axis, route)


def dft_tables(length):
    indices = jnp.arange(length, dtype=jnp.int32)
    turns = indices[:, None] * indices[None, :] % length
    angles = turns.astype(jnp.float32) * (2.0 * math.pi / length)
    cosine = jnp.cos(angles) / math.sqrt(length)
    sine = jnp.sin(angles) / math.sqrt(length)
    table_a = jnp.concatenate(
        [jnp.concatenate([cosine, sine], 1), jnp.concatenate([-sine, cosine], 1)], 0
    )
    table_b = jnp.concatenate(
        [jnp.concatenate([cosine, -sine], 1), jnp.concatenate([sine, cosine], 1)], 0
    )
    return (table_a.astype(jnp.bfloat16), table_b.astype(jnp.bfloat16))


def transforms(waves, left_table, right_table):
    length = waves[0][0].shape[0]
    stacked = [jnp.concatenate([part.astype(jnp.bfloat16) for part in wave], 0) for wave in waves]
    middles = [jnp.dot(left_table, s, preferred_element_type=jnp.float32) for s in stacked]
    middles = [m.astype(jnp.bfloat16) for m in middles]
    middles = [jnp.concatenate([m[:length], m[length:]], 1) for m in middles]
    results = [jnp.dot(m, right_table, preferred_element_type=jnp.float32) for m in middles]
    return [(r[:, :length], r[:, length:]) for r in results]


def product_of(left, right):
    return left[0] * right[0] - left[1] * right[1], left[0] * right[1] + left[1] * right[0]


def conj_product(left, right):
    return left[0] * right[0] + left[1] * right[1], left[1] * right[0] - left[0] * right[1]


def strip_copies(array, strips, row0, store, sem, outward):
    copies = []
    for s in range(array.shape[0]):
        for c in range(array.shape[1]):
            for k, strip in enumerate(strips):
                whole = array.at[s, c, :, pl.ds(k * lanes, lanes)]
                part = store.at[s, c, strip, pl.ds(row0, array.shape[2]), :]
                source, target = (part, whole) if outward else (whole, part)
                copies.append(pltpu.make_async_copy(source, target, sem))
    return copies


def run_copies(groups):
    copies = [copy for group in groups for copy in group]
    for copy in copies:
        copy.start()
    return copies


def process_slots(wanted, places, count, window, gradient, constants, todo):
    probe_ref, propagator_ref, measured_ref, table_a_ref, table_b_ref = constants
    length = probe_ref.shape[-1]
    halo_strips = length // lanes
    lane = lax.broadcasted_iota(jnp.int32, (length, lanes), 1)

    def pick(slot, found):
        chosen = jnp.logical_and(
            slot < count[0], wanted(places[2 * slot], places[2 * slot + 1])
        )

        @pl.when(chosen)
        def _():
            todo[found] = slot

        return found + chosen.astype(jnp.int32)

    found = lax.fori_loop(0, measured_ref.shape[0], pick, jnp.int32(0))

    def fetch(s, spot):
        row, strip, shift = spot
        back = lax.rem(lanes - shift, lanes)
        out = []
        for c in range(2):
            rolled = [
                pltpu.roll(window[s, c, strip + k, pl.ds(row, length), :], back, 1)
                for k in range(halo_strips + 1)
            ]
            parts = [
                jnp.where(lane < lanes - shift, rolled[k], rolled[k + 1])
                for k in range(halo_strips)
            ]
            out.append(jnp.concatenate(parts, 1))
        return tuple(out)

    def accumulate(s, spot, wave):
        row, strip, shift = spot
        for c in range(2):
            rolled = [
                pltpu.roll(wave[c][:, k * lanes : (k + 1) * lanes], shift, 1)
                for k in range(halo_strips)
            ]
            for k in range(halo_strips + 1):
                if k == 0:
                    part = jnp.where(lane >= shift, rolled[0], 0.0)
                elif k == halo_strips:
                    part = jnp.where(lane < shift, rolled[k - 1], 0.0)
                else:
                    part = jnp.where(lane < shift, rolled[k - 1], rolled[k])
                at = (s, c, strip + k, pl.ds(row, length), slice(None))
                gradient[at] = gradient[at] + part

    def run_slots(slots):
        table_a = table_a_ref[...]
        table_b = table_b_ref[...]
        spots = []
        for slot in slots:
            column = places[2 * slot + 1]
            spots.append((places[2 * slot], column // lanes, lax.rem(column, lanes)))
        probe = (probe_ref[0], probe_ref[1])
        propagator = (propagator_ref[0], propagator_ref[1])
        lits = [product_of(probe, fetch(0, spot)) for spot in spots]
        spreads = transforms(lits, table_a, table_b)
        spreads = transforms([product_of(propagator, w) for w in spreads], table_b, table_a)
        exits = [product_of(spread, fetch(1, spot)) for spread, spot in zip(spreads, spots)]
        fars = transforms(exits, table_a, table_b)
        residuals = []
        for far, slot in zip(fars, slots):
            power = far[0] * far[0] + far[1] * far[1]
            measured = measured_ref[slot].astype(jnp.float32)
            ratio = 1.0 - measured * jnp.minimum(lax.rsqrt(power), 1.0 / floor_value)
            residuals.append((far[0] * ratio, far[1] * ratio))
        backs = transforms(residuals, table_b, table_a)
        for back, spread, spot in zip(backs, spreads, spots):
            accumulate(1, spot, conj_product(back, spread))
        inners = [conj_product(back, fetch(1, spot)) for back, spot in zip(backs, spots)]
        inners = transforms(inners, table_a, table_b)
        firsts = transforms([conj_product(w, propagator) for w in inners], table_b, table_a)
        for first, spot in zip(firsts, spots):
            accumulate(0, spot, conj_product(first, probe))

    def pair(index, carry):
        run_slots([todo[2 * index], todo[2 * index + 1]])
        return carry

    lax.fori_loop(0, found // 2, pair, 0)

    @pl.when(lax.rem(found, 2) == 1)
    def _():
        run_slots([todo[found - 1]])


def sizes(object_shape, length):
    tile = object_shape[-1]
    own = range(tile // lanes)
    near = range(length // lanes)
    far = range(length // lanes, tile // lanes)
    past = range(tile // lanes, (tile + length) // lanes)
    return tile, own, near, far, past


def first_kernel(split, places, count, object_ref, *rest):
    constants, (window, gradient), (todo, sem) = rest[:5], rest[5:7], rest[7:]
    length = constants[0].shape[-1]
    tile, own, _, _, _ = sizes(object_ref.shape, length)
    loads = run_copies([strip_copies(object_ref, own, 0, window, sem, False)])
    gradient[...] = jnp.zeros_like(gradient)
    for copy in loads:
        copy.wait()

    def wanted(row, column):
        return jnp.logical_and(row <= tile - length, column <= tile - length)

    process_slots(wanted, places, count, window, gradient, constants, todo)


def second_kernel(split, places, count, near_ref, far_ref, corner_ref, right_ref, *rest):
    constants, (window, gradient), (todo, sem) = rest[:5], rest[7:9], rest[9:]
    length = constants[0].shape[-1]
    tile, _, near, far, past = sizes((right_ref.shape[2],), length)
    loads = run_copies(
        [
            strip_copies(near_ref, near, tile, window, sem, False),
            strip_copies(far_ref, far, tile, window, sem, False),
            strip_copies(corner_ref, past, tile, window, sem, False),
            strip_copies(right_ref, past, 0, window, sem, False),
        ]
    )
    for copy in loads:
        copy.wait()

    def wanted(row, column):
        early = jnp.logical_and(row <= tile - length, column <= tile - length)
        return jnp.logical_and(row <= tile - length + split, jnp.logical_not(early))

    process_slots(wanted, places, count, window, gradient, constants, todo)


def third_kernel(split, places, count, near_ref, far_ref, corner_ref, *rest):
    constants = rest[:5]
    near_out, far_out, corner_out, window, gradient, todo, sem = rest[7:]
    length = constants[0].shape[-1]
    tile, _, near, far, past = sizes((near_ref.shape[3] + far_ref.shape[3],), length)
    loads = run_copies(
        [
            strip_copies(near_ref, near, tile + split, window, sem, False),
            strip_copies(far_ref, far, tile + split, window, sem, False),
            strip_copies(corner_ref, past, tile + split, window, sem, False),
        ]
    )
    for copy in loads:
        copy.wait()

    def wanted(row, column):
        return row > tile - length + split

    process_slots(wanted, places, count, window, gradient, constants, todo)
    stores = run_copies(
        [
            strip_copies(corner_out, past, tile, gradient, sem, True),
            strip_copies(far_out, far, tile, gradient, sem, True),
            strip_copies(near_out, near, tile, gradient, sem, True),
        ]
    )
    for copy in stores:
        copy.wait()


def own_kernel(gradient, own_out, right_out, sem):
    _, own, _, _, past = sizes(own_out.shape, right_out.shape[-1])
    stores = run_copies(
        [
            strip_copies(right_out, past, 0, gradient, sem, True),
            strip_copies(own_out, own, 0, gradient, sem, True),
        ]
    )
    for copy in stores:
        copy.wait()


def add_kernel(column, gradient_in, piece_ref, gradient_out, held, added, sems):
    del gradient_in
    slices, parts, rows, columns = piece_ref.shape
    planes = [(s, c) for s in range(slices) for c in range(parts)]

    def spot(s, c):
        return gradient_out.at[s, c, pl.ds(0, rows), pl.ds(column, columns)]

    loads, pieces, stores = [], [], []
    for i, (s, c) in enumerate(planes):
        loads.append(pltpu.make_async_copy(spot(s, c), held.at[i], sems.at[0, i]))
        pieces.append(pltpu.make_async_copy(piece_ref.at[s, c], added.at[i], sems.at[1, i]))
        stores.append(pltpu.make_async_copy(held.at[i], spot(s, c), sems.at[2, i]))
        loads[i].start()
        pieces[i].start()
    for i in range(len(planes)):
        loads[i].wait()
        pieces[i].wait()
        held[i] = held[i] + added[i]
        stores[i].start()
    for store in stores:
        store.wait()


def add_piece(gradient, piece, column):
    slices, parts, rows, columns = piece.shape
    planes = slices * parts
    return pl.pallas_call(
        functools.partial(add_kernel, column),
        out_shape=jax.ShapeDtypeStruct(gradient.shape, gradient.dtype),
        in_specs=[any_space] * 2,
        out_specs=any_space,
        scratch_shapes=[pltpu.VMEM((planes, rows, columns), jnp.float32)] * 2
        + [pltpu.SemaphoreType.DMA((3, planes))],
        input_output_aliases={0: 0},
        compiler_params=pltpu.CompilerParams(vmem_limit_bytes=8 * 1024 * 1024),
    )(gradient, piece)


any_space = pl.BlockSpec(memory_space=pl.ANY)
hbm_space = pl.BlockSpec(memory_space=pltpu.HBM)
vmem_space = pl.BlockSpec(memory_space=pltpu.VMEM)
scalar_space = pl.BlockSpec(memory_space=pltpu.SMEM)


def slots_call(body, scalars, pieces, constants, state, state_shapes, out_shapes):
    first = len(scalars) + len(pieces) + len(constants)
    held = [pltpu.with_memory_space_constraint(x, pltpu.VMEM) for x in (*constants, *state)]
    aliases = {first + i: len(out_shapes) + i for i in range(len(state))}
    return pl.pallas_call(
        body,
        out_shape=[jax.ShapeDtypeStruct(s, jnp.float32) for s in out_shapes]
        + [pltpu.VMEM(s, jnp.float32) for s in state_shapes],
        in_specs=[scalar_space] * len(scalars)
        + [any_space if state else hbm_space] * len(pieces)
        + [vmem_space] * len(held),
        out_specs=[any_space] * len(out_shapes) + [vmem_space] * len(state_shapes),
        scratch_shapes=[
            pltpu.SMEM((constants[2].shape[0],), jnp.int32),
            pltpu.SemaphoreType.DMA,
        ],
        input_output_aliases=aliases,
        compiler_params=pltpu.CompilerParams(vmem_limit_bytes=20 * 1024 * 1024),
    )(*scalars, *pieces, *held)


def tile_gradient(object_field, probe_field, propagator_phase, positions, counts, amplitudes):
    length = probe_field.shape[-1]
    tile = object_field.shape[-1]
    split = length // 2
    slices, parts = object_field.shape[:2]
    top_near = object_field[:, :, :split, :length]
    top_far = object_field[:, :, :split, length:]
    top_near, top_far, later = lax.optimization_barrier((top_near, top_far, object_field))
    top_near = shifted(top_near, "row", -1)
    top_far = shifted(top_far, "row", -1)
    bottom_near = later[:, :, split:length, :length]
    bottom_far = later[:, :, split:length, length:]
    right = shifted(later[:, :, :, :length], "col", -1)
    bottom_near = shifted(bottom_near, "row", -1)
    bottom_far = shifted(bottom_far, "row", -1)
    top_corner = shifted(top_near, "col", -1)
    bottom_corner = shifted(bottom_near, "col", -1)
    propagator = jnp.stack([jnp.cos(propagator_phase), jnp.sin(propagator_phase)], 0)
    constants = (probe_field, propagator, amplitudes[0, 0], *dft_tables(length))
    scalars = (positions.reshape(-1), counts.reshape(-1))
    strips = (slices, parts, (tile + length) // lanes, tile + length, lanes)

    def call(kernel, pieces, state, out_shapes):
        body = functools.partial(kernel, split)
        return slots_call(body, scalars, pieces, constants, state, (strips, strips), out_shapes)

    state = call(first_kernel, (object_field,), (), ())
    state = call(second_kernel, (top_near, top_far, top_corner, right), state, ())
    lower_near, lower_far, corner, _, gradient = call(
        third_kernel,
        (bottom_near, bottom_far, bottom_corner),
        state,
        (
            (slices, parts, length, length),
            (slices, parts, length, tile - length),
            (slices, parts, length, length),
        ),
    )
    corner = shifted(corner, "col", 1)
    lower_far = shifted(lower_far, "row", 1)
    own, right = pl.pallas_call(
        own_kernel,
        name="own",
        out_shape=[
            jax.ShapeDtypeStruct(object_field.shape, jnp.float32),
            jax.ShapeDtypeStruct((slices, parts, tile, length), jnp.float32),
        ],
        in_specs=[vmem_space],
        out_specs=[any_space] * 2,
        scratch_shapes=[pltpu.SemaphoreType.DMA],
        compiler_params=pltpu.CompilerParams(vmem_limit_bytes=4 * 1024 * 1024),
    )(pltpu.with_memory_space_constraint(gradient, pltpu.VMEM))
    corner, right = lax.optimization_barrier((corner, right))
    lower_near = shifted(lower_near + corner, "row", 1)
    right = shifted(right, "col", 1)
    gradient = add_piece(own, right, 0)
    gradient = add_piece(gradient, lower_far, length)
    return add_piece(gradient, lower_near, 0)


def solution(mesh):
    return jax.shard_map(
        tile_gradient,
        mesh=mesh,
        in_specs=(
            P(None, None, "row", "col"),
            P(),
            P(),
            P("row", "col", None, None),
            P("row", "col"),
            P("row", "col", None, None, None),
        ),
        out_specs=P(None, None, "row", "col"),
        check_vma=False,
    )
```

```python
import functools
import math

import jax
import jax.numpy as jnp
from jax import lax
from jax.experimental import pallas as pl
from jax.experimental.pallas import tpu as pltpu
from jax.sharding import PartitionSpec as P


floor_value = 0.1
lanes = 128


def shifted(block, axis, distance):
    devices = range(lax.axis_size(axis))
    route = [((i - distance) % len(devices), i) for i in devices]
    return lax.ppermute(block, axis, route)


def dft_tables(length):
    indices = jnp.arange(length, dtype=jnp.int32)
    turns = indices[:, None] * indices[None, :] % length
    angles = turns.astype(jnp.float32) * (2.0 * math.pi / length)
    cosine = jnp.cos(angles) / math.sqrt(length)
    sine = jnp.sin(angles) / math.sqrt(length)
    table_a = jnp.concatenate(
        [jnp.concatenate([cosine, sine], 1), jnp.concatenate([-sine, cosine], 1)], 0
    )
    table_b = jnp.concatenate(
        [jnp.concatenate([cosine, -sine], 1), jnp.concatenate([sine, cosine], 1)], 0
    )
    return (table_a.astype(jnp.bfloat16), table_b.astype(jnp.bfloat16))


def sections(stacked, left_table, right_table):
    length = stacked.shape[1]
    middle = jnp.dot(left_table, stacked, preferred_element_type=jnp.float32)
    middle = middle.astype(jnp.bfloat16)
    middle = jnp.concatenate([middle[:length], middle[length:]], 1)
    result = jnp.dot(middle, right_table, preferred_element_type=jnp.float32)
    return result[:, :length], result[:, length:]


def transform(wave, left_table, right_table):
    stacked = jnp.concatenate([part.astype(jnp.bfloat16) for part in wave], 0)
    return sections(stacked, left_table, right_table)


def product_of(left, right):
    return left[0] * right[0] - left[1] * right[1], left[0] * right[1] + left[1] * right[0]


def conj_product(left, right):
    return left[0] * right[0] + left[1] * right[1], left[1] * right[0] - left[0] * right[1]


def strip_copies(array, strips, row0, store, plane, sem, outward):
    copies = []
    for s in range(array.shape[0]):
        for c in range(array.shape[1]):
            for k, strip in enumerate(strips):
                whole = array.at[s, c, :, pl.ds(k * lanes, lanes)]
                part = store.at[plane + s, c, strip, pl.ds(row0, array.shape[2]), :]
                source, target = (part, whole) if outward else (whole, part)
                copies.append(pltpu.make_async_copy(source, target, sem))
    return copies


def run_copies(groups):
    copies = [copy for group in groups for copy in group]
    for copy in copies:
        copy.start()
    return copies


def finish(copies):
    for copy in copies:
        copy.wait()


def patch_spot(places, slot):
    column = places[2 * slot + 1]
    return places[2 * slot], column // lanes, lax.rem(column, lanes)


def fetch(window, s, spot, length):
    row, strip, shift = spot
    back = lax.rem(lanes - shift, lanes)
    lane = lax.broadcasted_iota(jnp.int32, (length, lanes), 1)
    out = []
    for c in range(2):
        rolled = [
            pltpu.roll(window[s, c, strip + k, pl.ds(row, length), :], back, 1)
            for k in range(length // lanes + 1)
        ]
        parts = [
            jnp.where(lane < lanes - shift, rolled[k], rolled[k + 1])
            for k in range(length // lanes)
        ]
        out.append(jnp.concatenate(parts, 1))
    return tuple(out)


def accumulate(gradient, s, spot, wave, length):
    row, strip, shift = spot
    lane = lax.broadcasted_iota(jnp.int32, (length, lanes), 1)
    count = length // lanes
    for c in range(2):
        rolled = [
            pltpu.roll(wave[c][:, k * lanes : (k + 1) * lanes], shift, 1) for k in range(count)
        ]
        for k in range(count + 1):
            if k == 0:
                part = jnp.where(lane >= shift, rolled[0], 0.0)
            elif k == count:
                part = jnp.where(lane < shift, rolled[k - 1], 0.0)
            else:
                part = jnp.where(lane < shift, rolled[k - 1], rolled[k])
            at = (s, c, strip + k, pl.ds(row, length), slice(None))
            gradient[at] = gradient[at] + part


def spread_slot(places, window, constants, spreads, slot):
    probe, propagator, _, table_a, table_b = constants
    length = probe.shape[-1]
    lit = product_of((probe[0], probe[1]), fetch(window, 0, patch_spot(places, slot), length))
    wave = transform(lit, table_a[...], table_b[...])
    wave = product_of((propagator[0], propagator[1]), wave)
    wave = transform(wave, table_b[...], table_a[...])
    spreads[slot, 0] = wave[0]
    spreads[slot, 1] = wave[1]


def back_slot(places, window, gradient, constants, spreads, inners, slot):
    probe, _, measured_ref, table_a, table_b = constants
    length = probe.shape[-1]
    spot = patch_spot(places, slot)
    second = fetch(window, 1, spot, length)
    spread = (spreads[slot, 0], spreads[slot, 1])
    far = transform(product_of(spread, second), table_a[...], table_b[...])
    power = far[0] * far[0] + far[1] * far[1]
    measured = measured_ref[slot].astype(jnp.float32)
    ratio = 1.0 - measured * jnp.minimum(lax.rsqrt(power), 1.0 / floor_value)
    back = transform((far[0] * ratio, far[1] * ratio), table_b[...], table_a[...])
    inner = conj_product(back, second)
    inners[slot, pl.ds(0, length), :] = inner[0].astype(jnp.bfloat16)
    inners[slot, pl.ds(length, length), :] = inner[1].astype(jnp.bfloat16)
    spread = (spreads[slot, 0], spreads[slot, 1])
    accumulate(gradient, 1, spot, conj_product(back, spread), length)


def first_slot(places, gradient, constants, inners, slot):
    probe, propagator, _, table_a, table_b = constants
    length = probe.shape[-1]
    wave = sections(inners[slot], table_a[...], table_b[...])
    wave = conj_product(wave, (propagator[0], propagator[1]))
    wave = transform(wave, table_b[...], table_a[...])
    grad = conj_product(wave, (probe[0], probe[1]))
    accumulate(gradient, 0, patch_spot(places, slot), grad, length)


def each_slot(places, count, tile, length, inside, visit):
    def step(slot, carry):
        within = jnp.logical_and(
            places[2 * slot] <= tile - length, places[2 * slot + 1] <= tile - length
        )
        if inside is None:
            visit(slot)
        else:

            @pl.when(within if inside else jnp.logical_not(within))
            def _():
                visit(slot)

        return carry

    lax.fori_loop(0, count[0], step, 0)


def sizes(tile, length):
    own = range(tile // lanes)
    near = range(length // lanes)
    far = range(length // lanes, tile // lanes)
    past = range(tile // lanes, (tile + length) // lanes)
    return own, near, far, past


def own_slots_kernel(places, count, object_ref, *rest):
    constants, (window, gradient, spreads, inners, sem) = rest[:5], rest[5:]
    length = constants[0].shape[-1]
    tile = object_ref.shape[-1]
    own, _, _, _ = sizes(tile, length)
    loads = run_copies([strip_copies(object_ref, own, 0, window, 0, sem, False)])
    gradient[...] = jnp.zeros_like(gradient)
    finish(loads)

    def visit(slot):
        spread_slot(places, window, constants, spreads, slot)
        back_slot(places, window, gradient, constants, spreads, inners, slot)

    each_slot(places, count, tile, length, True, visit)


def spread_kernel(places, count, near_ref, far_ref, corner_ref, right_ref, *rest):
    constants, (window, gradient, spreads, inners, sem) = rest[:5], rest[9:]
    length = constants[0].shape[-1]
    tile = right_ref.shape[2]
    _, near, far, past = sizes(tile, length)
    finish(
        run_copies(
            [
                strip_copies(near_ref, near, tile, window, 0, sem, False),
                strip_copies(far_ref, far, tile, window, 0, sem, False),
                strip_copies(corner_ref, past, tile, window, 0, sem, False),
                strip_copies(right_ref, past, 0, window, 0, sem, False),
            ]
        )
    )

    def visit(slot):
        spread_slot(places, window, constants, spreads, slot)

    each_slot(places, count, tile, length, False, visit)


def load_kernel(near_ref, corner_ref, right_ref, window_in, window, sem):
    del window_in
    length = near_ref.shape[3]
    tile = right_ref.shape[2]
    _, near, _, past = sizes(tile, length)
    finish(
        run_copies(
            [
                strip_copies(near_ref, near, tile, window, 1, sem, False),
                strip_copies(corner_ref, past, tile, window, 1, sem, False),
                strip_copies(right_ref, past, 0, window, 1, sem, False),
            ]
        )
    )


def back_kernel(places, count, far_ref, *rest):
    constants = rest[:5]
    near_out, far_out, corner_out, window, gradient, spreads, inners, sem = rest[9:]
    length = constants[0].shape[-1]
    tile = length + far_ref.shape[3]
    _, near, far, past = sizes(tile, length)
    finish(run_copies([strip_copies(far_ref, far, tile, window, 1, sem, False)]))

    def visit(slot):
        back_slot(places, window, gradient, constants, spreads, inners, slot)

    each_slot(places, count, tile, length, False, visit)
    finish(
        run_copies(
            [
                strip_copies(corner_out, past, tile, gradient, 1, sem, True),
                strip_copies(far_out, far, tile, gradient, 1, sem, True),
                strip_copies(near_out, near, tile, gradient, 1, sem, True),
            ]
        )
    )


def first_kernel(places, count, *rest):
    constants = rest[:5]
    near_out, far_out, corner_out, _, gradient, _, inners, sem = rest[9:]
    length = constants[0].shape[-1]
    tile = length + far_out.shape[3]
    _, near, far, past = sizes(tile, length)

    def visit(slot):
        first_slot(places, gradient, constants, inners, slot)

    each_slot(places, count, tile, length, None, visit)
    finish(
        run_copies(
            [
                strip_copies(corner_out, past, tile, gradient, 0, sem, True),
                strip_copies(far_out, far, tile, gradient, 0, sem, True),
                strip_copies(near_out, near, tile, gradient, 0, sem, True),
            ]
        )
    )


def own_kernel(gradient, own_out, right_out, sem):
    tile = own_out.shape[-1]
    own, _, _, past = sizes(tile, right_out.shape[-1])
    finish(
        run_copies(
            [
                strip_copies(right_out, past, 0, gradient, 0, sem, True),
                strip_copies(own_out, own, 0, gradient, 0, sem, True),
            ]
        )
    )


def add_kernel(plane, column, gradient_in, piece_ref, gradient_out, held, added, sems):
    del gradient_in
    slices, parts, rows, columns = piece_ref.shape
    planes = [(s, c) for s in range(slices) for c in range(parts)]

    def spot(s, c):
        return gradient_out.at[plane + s, c, pl.ds(0, rows), pl.ds(column, columns)]

    loads, pieces, stores = [], [], []
    for i, (s, c) in enumerate(planes):
        loads.append(pltpu.make_async_copy(spot(s, c), held.at[i], sems.at[0, i]))
        pieces.append(pltpu.make_async_copy(piece_ref.at[s, c], added.at[i], sems.at[1, i]))
        stores.append(pltpu.make_async_copy(held.at[i], spot(s, c), sems.at[2, i]))
        loads[i].start()
        pieces[i].start()
    for i in range(len(planes)):
        loads[i].wait()
        pieces[i].wait()
        held[i] = held[i] + added[i]
        stores[i].start()
    finish(stores)


def add_piece(gradient, piece, plane, column):
    slices, parts, rows, columns = piece.shape
    planes = slices * parts
    return pl.pallas_call(
        functools.partial(add_kernel, plane, column),
        out_shape=jax.ShapeDtypeStruct(gradient.shape, gradient.dtype),
        in_specs=[any_space] * 2,
        out_specs=any_space,
        scratch_shapes=[pltpu.VMEM((planes, rows, columns), jnp.float32)] * 2
        + [pltpu.SemaphoreType.DMA((3, planes))],
        input_output_aliases={0: 0},
        compiler_params=pltpu.CompilerParams(vmem_limit_bytes=8 * 1024 * 1024),
    )(gradient, piece)


def in_vmem(x):
    return pltpu.with_memory_space_constraint(x, pltpu.VMEM)


any_space = pl.BlockSpec(memory_space=pl.ANY)
hbm_space = pl.BlockSpec(memory_space=pltpu.HBM)
vmem_space = pl.BlockSpec(memory_space=pltpu.VMEM)
scalar_space = pl.BlockSpec(memory_space=pltpu.SMEM)


def slots_call(body, scalars, pieces, constants, state, state_types, out_shapes):
    first = len(scalars) + len(pieces) + len(constants)
    aliases = {first + i: len(out_shapes) + i for i in range(len(state))}
    return pl.pallas_call(
        body,
        out_shape=[jax.ShapeDtypeStruct(s, jnp.float32) for s in out_shapes] + state_types,
        in_specs=[scalar_space] * len(scalars)
        + [any_space if state else hbm_space] * len(pieces)
        + [vmem_space] * (len(constants) + len(state)),
        out_specs=[any_space] * len(out_shapes) + [vmem_space] * len(state_types),
        scratch_shapes=[pltpu.SemaphoreType.DMA],
        input_output_aliases=aliases,
        compiler_params=pltpu.CompilerParams(vmem_limit_bytes=20 * 1024 * 1024),
    )(*scalars, *pieces, *[in_vmem(x) for x in (*constants, *state)])


def tile_gradient(object_field, probe_field, propagator_phase, positions, counts, amplitudes):
    length = probe_field.shape[-1]
    tile = object_field.shape[-1]
    slices, parts = object_field.shape[:2]
    slots = positions.shape[-2]

    near0 = object_field[:1, :, :length, :length]
    near0, source = lax.optimization_barrier((near0, object_field))
    near0 = shifted(near0, "row", -1)
    right0 = source[:1, :, :, :length]
    far0 = source[:1, :, :length, length:]
    right0, far0, source = lax.optimization_barrier((right0, far0, source))
    right0 = shifted(right0, "col", -1)
    far0 = shifted(far0, "row", -1)
    near1 = shifted(source[1:, :, :length, :length], "row", -1)
    far1 = shifted(source[1:, :, :length, length:], "row", -1)
    right1 = shifted(source[1:, :, :, :length], "col", -1)
    corner0 = shifted(near0, "col", -1)
    corner1 = shifted(near1, "col", -1)

    propagator = jnp.stack([jnp.cos(propagator_phase), jnp.sin(propagator_phase)], 0)
    constants = (probe_field, propagator, amplitudes[0, 0], *dft_tables(length))
    scalars = (positions.reshape(-1), counts.reshape(-1))
    strips = (slices, parts, (tile + length) // lanes, tile + length, lanes)
    state_types = [
        pltpu.VMEM(strips, jnp.float32),
        pltpu.VMEM(strips, jnp.float32),
        pltpu.VMEM((slots, parts, length, length), jnp.float32),
        pltpu.VMEM((slots, parts * length, length), jnp.bfloat16),
    ]
    piece_shapes = (
        (1, parts, length, length),
        (1, parts, length, tile - length),
        (1, parts, length, length),
    )

    def call(kernel, pieces, state, out_shapes):
        return slots_call(kernel, scalars, pieces, constants, state, state_types, out_shapes)

    state = call(own_slots_kernel, (object_field,), (), ())
    state = call(spread_kernel, (near0, far0, corner0, right0), state, ())
    window, *others = state
    window = pl.pallas_call(
        load_kernel,
        name="load_halo",
        out_shape=state_types[0],
        in_specs=[any_space] * 3 + [vmem_space],
        out_specs=vmem_space,
        scratch_shapes=[pltpu.SemaphoreType.DMA],
        input_output_aliases={3: 0},
        compiler_params=pltpu.CompilerParams(vmem_limit_bytes=4 * 1024 * 1024),
    )(near1, corner1, right1, in_vmem(window))
    near1, far1, corner1, *state = call(back_kernel, (far1,), (window, *others), piece_shapes)
    corner1 = shifted(corner1, "col", 1)
    far1 = shifted(far1, "row", 1)
    near0, far0, corner0, window, gradient, *_ = call(first_kernel, (), state, piece_shapes)
    near1 = shifted(near1 + corner1, "row", 1)
    corner0 = shifted(corner0, "col", 1)
    far0 = shifted(far0, "row", 1)
    own, right = pl.pallas_call(
        own_kernel,
        name="own",
        out_shape=[
            jax.ShapeDtypeStruct(object_field.shape, jnp.float32),
            jax.ShapeDtypeStruct((slices, parts, tile, length), jnp.float32),
        ],
        in_specs=[vmem_space],
        out_specs=[any_space] * 2,
        scratch_shapes=[pltpu.SemaphoreType.DMA],
        compiler_params=pltpu.CompilerParams(vmem_limit_bytes=4 * 1024 * 1024),
    )(in_vmem(gradient))
    corner0, right = lax.optimization_barrier((corner0, right))
    near0 = shifted(near0 + corner0, "row", 1)
    right = shifted(right, "col", 1)
    result = add_piece(own, far1, 1, length)
    result = add_piece(result, near1, 1, 0)
    result = add_piece(result, right, 0, 0)
    result = add_piece(result, far0, 0, length)
    return add_piece(result, near0, 0, 0)


def solution(mesh):
    return jax.shard_map(
        tile_gradient,
        mesh=mesh,
        in_specs=(
            P(None, None, "row", "col"),
            P(),
            P(),
            P("row", "col", None, None),
            P("row", "col"),
            P("row", "col", None, None, None),
        ),
        out_specs=P(None, None, "row", "col"),
        check_vma=False,
    )
```

```python
import functools
import math

import jax
import jax.numpy as jnp
import numpy as np
from jax import lax
from jax.experimental import pallas as pl
from jax.experimental.pallas import tpu as pltpu
from jax.sharding import PartitionSpec as P


floor_value = 0.1
lanes = 128


def shifted(block, axis, distance):
    devices = range(lax.axis_size(axis))
    route = [((i - distance) % len(devices), i) for i in devices]
    return lax.ppermute(block, axis, route)


def dft_tables(length):
    indices = np.arange(length, dtype=np.int32)
    turns = indices[:, None] * indices[None, :] % length
    angles = turns.astype(np.float32) * np.float32(2.0 * math.pi / length)
    cosine = np.cos(angles) / np.float32(math.sqrt(length))
    sine = np.sin(angles) / np.float32(math.sqrt(length))
    table_a = np.block([[cosine, sine], [-sine, cosine]])
    table_b = np.block([[cosine, -sine], [sine, cosine]])
    return (jnp.asarray(table_a, jnp.bfloat16), jnp.asarray(table_b, jnp.bfloat16))


def sections(stacked, left_table, right_table):
    length = stacked[0].shape[1]
    middle = [
        jnp.dot(left_table, wave, preferred_element_type=jnp.float32).astype(jnp.bfloat16)
        for wave in stacked
    ]
    middle = [jnp.concatenate([wave[:length], wave[length:]], 1) for wave in middle]
    result = [
        jnp.dot(wave, right_table, preferred_element_type=jnp.float32) for wave in middle
    ]
    return [(wave[:, :length], wave[:, length:]) for wave in result]


def transforms(waves, left_table, right_table):
    stacked = [
        jnp.concatenate([part.astype(jnp.bfloat16) for part in wave], 0) for wave in waves
    ]
    return sections(stacked, left_table, right_table)


def product_of(left, right):
    return left[0] * right[0] - left[1] * right[1], left[0] * right[1] + left[1] * right[0]


def conj_product(left, right):
    return left[0] * right[0] + left[1] * right[1], left[1] * right[0] - left[0] * right[1]


def strip_copies(array, strips, row0, store, plane, sem, outward):
    copies = []
    for s in range(array.shape[0]):
        for c in range(array.shape[1]):
            for k, strip in enumerate(strips):
                whole = array.at[s, c, :, pl.ds(k * lanes, lanes)]
                part = store.at[plane + s, c, strip, pl.ds(row0, array.shape[2]), :]
                source, target = (part, whole) if outward else (whole, part)
                copies.append(pltpu.make_async_copy(source, target, sem))
    return copies


def run_copies(groups):
    copies = [copy for group in groups for copy in group]
    for copy in copies:
        copy.start()
    return copies


def finish(copies):
    for copy in copies:
        copy.wait()


def patch_spot(places, slot):
    column = places[2 * slot + 1]
    return places[2 * slot], column // lanes, lax.rem(column, lanes)


def fetch(window, s, spot, length):
    row, strip, shift = spot
    back = lax.rem(lanes - shift, lanes)
    lane = lax.broadcasted_iota(jnp.int32, (length, lanes), 1)
    out = []
    for c in range(2):
        rolled = [
            pltpu.roll(window[s, c, strip + k, pl.ds(row, length), :], back, 1)
            for k in range(length // lanes + 1)
        ]
        parts = [
            jnp.where(lane < lanes - shift, rolled[k], rolled[k + 1])
            for k in range(length // lanes)
        ]
        out.append(jnp.concatenate(parts, 1))
    return tuple(out)


def accumulate(gradient, s, spot, wave, length):
    row, strip, shift = spot
    lane = lax.broadcasted_iota(jnp.int32, (length, lanes), 1)
    count = length // lanes
    for c in range(2):
        rolled = [
            pltpu.roll(wave[c][:, k * lanes : (k + 1) * lanes], shift, 1) for k in range(count)
        ]
        for k in range(count + 1):
            if k == 0:
                part = jnp.where(lane >= shift, rolled[0], 0.0)
            elif k == count:
                part = jnp.where(lane < shift, rolled[k - 1], 0.0)
            else:
                part = jnp.where(lane < shift, rolled[k - 1], rolled[k])
            at = (s, c, strip + k, pl.ds(row, length), slice(None))
            gradient[at] = gradient[at] + part


def spread_slots(places, window, constants, spreads, slots):
    probe, propagator, _, table_a, table_b = constants
    length = probe.shape[-1]
    waves = [
        product_of((probe[0], probe[1]), fetch(window, 0, patch_spot(places, slot), length))
        for slot in slots
    ]
    waves = transforms(waves, table_a[...], table_b[...])
    waves = [product_of((propagator[0], propagator[1]), wave) for wave in waves]
    waves = transforms(waves, table_b[...], table_a[...])
    for wave, slot in zip(waves, slots):
        spreads[slot, 0] = wave[0]
        spreads[slot, 1] = wave[1]


def back_slots(places, window, gradient, constants, spreads, inners, slots):
    probe, _, measured_ref, table_a, table_b = constants
    length = probe.shape[-1]
    spots = [patch_spot(places, slot) for slot in slots]
    waves = [
        product_of((spreads[slot, 0], spreads[slot, 1]), fetch(window, 1, spot, length))
        for slot, spot in zip(slots, spots)
    ]
    residuals = []
    for far, slot in zip(transforms(waves, table_a[...], table_b[...]), slots):
        power = far[0] * far[0] + far[1] * far[1]
        measured = measured_ref[slot].astype(jnp.float32)
        ratio = 1.0 - measured * jnp.minimum(lax.rsqrt(power), 1.0 / floor_value)
        residuals.append((far[0] * ratio, far[1] * ratio))
    backs = transforms(residuals, table_b[...], table_a[...])
    for back, slot, spot in zip(backs, slots, spots):
        inner = conj_product(back, fetch(window, 1, spot, length))
        inners[slot, pl.ds(0, length), :] = inner[0].astype(jnp.bfloat16)
        inners[slot, pl.ds(length, length), :] = inner[1].astype(jnp.bfloat16)
        spread = (spreads[slot, 0], spreads[slot, 1])
        accumulate(gradient, 1, spot, conj_product(back, spread), length)


def first_slots(places, gradient, constants, inners, slots):
    probe, propagator, _, table_a, table_b = constants
    length = probe.shape[-1]
    waves = sections([inners[slot] for slot in slots], table_a[...], table_b[...])
    waves = [conj_product(wave, (propagator[0], propagator[1])) for wave in waves]
    waves = transforms(waves, table_b[...], table_a[...])
    for wave, slot in zip(waves, slots):
        grad = conj_product(wave, (probe[0], probe[1]))
        accumulate(gradient, 0, patch_spot(places, slot), grad, length)


def visit_slots(places, count, slots, limit, inside, todo, exact, visit):
    def pick(slot, found):
        within = jnp.logical_and(places[2 * slot] <= limit, places[2 * slot + 1] <= limit)
        chosen = slot < count[0]
        if inside is not None:
            chosen = jnp.logical_and(chosen, within == inside)

        @pl.when(chosen)
        def _():
            todo[found] = slot

        return found + chosen.astype(jnp.int32)

    found = lax.fori_loop(0, slots, pick, jnp.int32(0))
    if exact:
        for size in range(1, slots + 1):

            @pl.when(found == size)
            def _():
                visit([todo[i] for i in range(size)])

        return

    def pair(index, carry):
        visit([todo[2 * index], todo[2 * index + 1]])
        return carry

    lax.fori_loop(0, found // 2, pair, 0)

    @pl.when(lax.rem(found, 2) == 1)
    def _():
        visit([todo[found - 1]])


def sizes(tile, length):
    own = range(tile // lanes)
    near = range(length // lanes)
    far = range(length // lanes, tile // lanes)
    past = range(tile // lanes, (tile + length) // lanes)
    return own, near, far, past


def from_strips(out, strips, row0, store, plane):
    for c in range(out.shape[1]):
        for k, strip in enumerate(strips):
            out[0, c, :, pl.ds(k * lanes, lanes)] = store[
                plane, c, strip, pl.ds(row0, out.shape[2]), :
            ]


def into_strips(piece, strips, row0, store, plane):
    for c in range(piece.shape[1]):
        for k, strip in enumerate(strips):
            store[plane, c, strip, pl.ds(row0, piece.shape[2]), :] = piece[
                0, c, :, pl.ds(k * lanes, lanes)
            ]


def pack_kernel(corners, object_ref, *rest):
    outs, sem = rest[:-1], rest[-1]
    copies = []
    for (s, row, column), out in zip(corners, outs):
        for c in range(out.shape[1]):
            piece = object_ref.at[
                s, c, pl.ds(row, out.shape[2]), pl.ds(column, out.shape[3])
            ]
            copies.append(pltpu.make_async_copy(piece, out.at[0, c], sem))
    for copy in copies:
        copy.start()
    finish(copies)


def pack(object_field, pieces):
    return pl.pallas_call(
        functools.partial(pack_kernel, [piece[:3] for piece in pieces]),
        out_shape=[
            jax.ShapeDtypeStruct((1, object_field.shape[1], *piece[3:]), jnp.float32)
            for piece in pieces
        ],
        in_specs=[hbm_space],
        out_specs=[any_space] * len(pieces),
        scratch_shapes=[pltpu.SemaphoreType.DMA],
        compiler_params=pltpu.CompilerParams(vmem_limit_bytes=1024 * 1024),
    )(in_hbm(object_field))


def own_slots_kernel(places, count, object_ref, *rest):
    constants, (window, gradient, spreads, inners, todo, sem) = rest[:5], rest[5:]
    length = constants[0].shape[-1]
    tile = object_ref.shape[-1]
    own, _, _, _ = sizes(tile, length)
    loads = run_copies([strip_copies(object_ref, own, 0, window, 0, sem, False)])
    gradient[...] = jnp.zeros_like(gradient)
    finish(loads)

    def visit(slots):
        spread_slots(places, window, constants, spreads, slots)
        back_slots(places, window, gradient, constants, spreads, inners, slots)

    visit_slots(
        places, count, inners.shape[0], tile - length, True, todo, False, visit
    )


def spread_kernel(places, count, near_ref, far_ref, corner_ref, right_ref, *rest):
    constants, (window, gradient, spreads, inners, todo, sem) = rest[:5], rest[9:]
    length = constants[0].shape[-1]
    tile = right_ref.shape[2]
    _, near, far, past = sizes(tile, length)
    finish(
        run_copies(
            [
                strip_copies(near_ref, near, tile, window, 0, sem, False),
                strip_copies(far_ref, far, tile, window, 0, sem, False),
                strip_copies(corner_ref, past, tile, window, 0, sem, False),
                strip_copies(right_ref, past, 0, window, 0, sem, False),
            ]
        )
    )

    def visit(slots):
        spread_slots(places, window, constants, spreads, slots)

    visit_slots(
        places, count, inners.shape[0], tile - length, False, todo, False, visit
    )


def load_kernel(near_ref, corner_ref, right_ref, window_in, window, sem):
    del window_in
    length = near_ref.shape[3]
    tile = right_ref.shape[2]
    _, near, _, past = sizes(tile, length)
    finish(
        run_copies(
            [
                strip_copies(near_ref, near, tile, window, 1, sem, False),
                strip_copies(corner_ref, past, tile, window, 1, sem, False),
                strip_copies(right_ref, past, 0, window, 1, sem, False),
            ]
        )
    )


def back_kernel(places, count, far_ref, *rest):
    constants = rest[:5]
    near_out, far_out, corner_out, window, gradient, spreads, inners, todo, _ = rest[9:]
    length = constants[0].shape[-1]
    tile = length + far_ref.shape[3]
    _, near, far, past = sizes(tile, length)
    into_strips(far_ref, far, tile, window, 1)

    def visit(slots):
        back_slots(places, window, gradient, constants, spreads, inners, slots)

    visit_slots(
        places, count, inners.shape[0], tile - length, False, todo, True, visit
    )
    from_strips(corner_out, past, tile, gradient, 1)
    from_strips(far_out, far, tile, gradient, 1)
    from_strips(near_out, near, tile, gradient, 1)


def first_kernel(places, count, *rest):
    constants = rest[:5]
    near_out, far_out, corner_out, _, gradient, _, inners, todo, _ = rest[9:]
    length = constants[0].shape[-1]
    tile = length + far_out.shape[3]
    _, near, far, past = sizes(tile, length)

    def visit(slots):
        first_slots(places, gradient, constants, inners, slots)

    visit_slots(
        places, count, inners.shape[0], tile - length, None, todo, False, visit
    )
    from_strips(corner_out, past, tile, gradient, 0)
    from_strips(far_out, far, tile, gradient, 0)
    from_strips(near_out, near, tile, gradient, 0)


def own_kernel(gradient, own_out, right_out, sem):
    tile = own_out.shape[-1]
    own, _, _, past = sizes(tile, right_out.shape[-1])
    finish(
        run_copies(
            [
                strip_copies(right_out, past, 0, gradient, 0, sem, True),
                strip_copies(own_out, own, 0, gradient, 0, sem, True),
            ]
        )
    )


def add_kernel(plane, column, gradient_in, piece_ref, gradient_out, held, added, sems):
    del gradient_in
    slices, parts, rows, columns = piece_ref.shape
    planes = [(s, c) for s in range(slices) for c in range(parts)]

    def spot(s, c):
        return gradient_out.at[plane + s, c, pl.ds(0, rows), pl.ds(column, columns)]

    loads, pieces, stores = [], [], []
    for i, (s, c) in enumerate(planes):
        loads.append(pltpu.make_async_copy(spot(s, c), held.at[i], sems.at[0, i]))
        pieces.append(pltpu.make_async_copy(piece_ref.at[s, c], added.at[i], sems.at[1, i]))
        stores.append(pltpu.make_async_copy(held.at[i], spot(s, c), sems.at[2, i]))
        loads[i].start()
        pieces[i].start()
    for i in range(len(planes)):
        loads[i].wait()
        pieces[i].wait()
        held[i] = held[i] + added[i]
        stores[i].start()
    finish(stores)


def add_piece(gradient, piece, plane, column):
    slices, parts, rows, columns = piece.shape
    planes = slices * parts
    return pl.pallas_call(
        functools.partial(add_kernel, plane, column),
        out_shape=jax.ShapeDtypeStruct(gradient.shape, gradient.dtype),
        in_specs=[any_space] * 2,
        out_specs=any_space,
        scratch_shapes=[pltpu.VMEM((planes, rows, columns), jnp.float32)] * 2
        + [pltpu.SemaphoreType.DMA((3, planes))],
        input_output_aliases={0: 0},
        compiler_params=pltpu.CompilerParams(vmem_limit_bytes=8 * 1024 * 1024),
    )(gradient, piece)


def in_hbm(x):
    return pltpu.with_memory_space_constraint(x, pltpu.HBM)


def in_vmem(x):
    return pltpu.with_memory_space_constraint(x, pltpu.VMEM)


any_space = pl.BlockSpec(memory_space=pl.ANY)
hbm_space = pl.BlockSpec(memory_space=pltpu.HBM)
vmem_space = pl.BlockSpec(memory_space=pltpu.VMEM)
scalar_space = pl.BlockSpec(memory_space=pltpu.SMEM)


def slots_call(body, scalars, pieces, constants, state, state_types, out_shapes):
    first = len(scalars) + len(pieces) + len(constants)
    aliases = {first + i: len(out_shapes) + i for i in range(len(state))}
    close = bool(out_shapes)
    if close:
        pieces = [in_vmem(piece) for piece in pieces]
    piece_space = vmem_space if close else any_space if state else hbm_space
    return pl.pallas_call(
        body,
        out_shape=[pltpu.VMEM(s, jnp.float32) for s in out_shapes] + state_types,
        in_specs=[scalar_space] * len(scalars)
        + [piece_space] * len(pieces)
        + [vmem_space] * (len(constants) + len(state)),
        out_specs=[vmem_space] * (len(out_shapes) + len(state_types)),
        scratch_shapes=[
            pltpu.SMEM((constants[2].shape[0],), jnp.int32),
            pltpu.SemaphoreType.DMA,
        ],
        input_output_aliases=aliases,
        compiler_params=pltpu.CompilerParams(vmem_limit_bytes=20 * 1024 * 1024),
    )(*scalars, *pieces, *[in_vmem(x) for x in (*constants, *state)])


def tile_gradient(object_field, probe_field, propagator_phase, positions, counts, amplitudes):
    length = probe_field.shape[-1]
    tile = object_field.shape[-1]
    slices, parts = object_field.shape[:2]
    slots = positions.shape[-2]

    rest = tile - length
    (near0,) = pack(object_field, [(0, 0, 0, length, length)])
    right0, far0, near1, far1, right1 = pack(
        object_field,
        [
            (0, 0, 0, tile, length),
            (0, 0, length, length, rest),
            (1, 0, 0, length, length),
            (1, 0, length, length, rest),
            (1, 0, 0, tile, length),
        ],
    )
    near0 = shifted(near0, "row", -1)
    right0 = shifted(right0, "col", -1)
    far0 = shifted(far0, "row", -1)
    near1 = shifted(near1, "row", -1)
    far1 = shifted(far1, "row", -1)
    right1 = shifted(right1, "col", -1)
    corner0 = shifted(near0, "col", -1)
    corner1 = shifted(near1, "col", -1)

    propagator = jnp.stack([jnp.cos(propagator_phase), jnp.sin(propagator_phase)], 0)
    constants = (probe_field, propagator, amplitudes[0, 0], *dft_tables(length))
    scalars = (positions.reshape(-1), counts.reshape(-1))
    strips = (slices, parts, (tile + length) // lanes, tile + length, lanes)
    state_types = [
        pltpu.VMEM(strips, jnp.float32),
        pltpu.VMEM(strips, jnp.float32),
        pltpu.VMEM((slots, parts, length, length), jnp.float32),
        pltpu.VMEM((slots, parts * length, length), jnp.bfloat16),
    ]
    piece_shapes = (
        (1, parts, length, length),
        (1, parts, length, tile - length),
        (1, parts, length, length),
    )

    def call(kernel, pieces, state, out_shapes):
        return slots_call(kernel, scalars, pieces, constants, state, state_types, out_shapes)

    state = call(own_slots_kernel, (in_hbm(object_field),), (), ())
    state = call(spread_kernel, (near0, far0, corner0, right0), state, ())
    window, *others = state
    window = pl.pallas_call(
        load_kernel,
        name="load_halo",
        out_shape=state_types[0],
        in_specs=[any_space] * 3 + [vmem_space],
        out_specs=vmem_space,
        scratch_shapes=[pltpu.SemaphoreType.DMA],
        input_output_aliases={3: 0},
        compiler_params=pltpu.CompilerParams(vmem_limit_bytes=4 * 1024 * 1024),
    )(near1, corner1, right1, in_vmem(window))
    near1, far1, corner1, *state = call(back_kernel, (far1,), (window, *others), piece_shapes)
    corner1 = shifted(corner1, "col", 1)
    far1 = shifted(far1, "row", 1)
    near0, far0, corner0, window, gradient, *_ = call(first_kernel, (), state, piece_shapes)
    near1 = shifted(near1 + corner1, "row", 1)
    corner0 = shifted(corner0, "col", 1)
    far0 = shifted(far0, "row", 1)
    own, right = pl.pallas_call(
        own_kernel,
        name="own",
        out_shape=[
            jax.ShapeDtypeStruct(object_field.shape, jnp.float32),
            jax.ShapeDtypeStruct((slices, parts, tile, length), jnp.float32),
        ],
        in_specs=[vmem_space],
        out_specs=[any_space] * 2,
        scratch_shapes=[pltpu.SemaphoreType.DMA],
        compiler_params=pltpu.CompilerParams(vmem_limit_bytes=4 * 1024 * 1024),
    )(in_vmem(gradient))
    corner0, right = lax.optimization_barrier((corner0, right))
    near0 = shifted(near0 + corner0, "row", 1)
    right = shifted(right, "col", 1)
    result = add_piece(own, far1, 1, length)
    result = add_piece(result, near1, 1, 0)
    result = add_piece(result, right, 0, 0)
    result = add_piece(result, far0, 0, length)
    return add_piece(result, near0, 0, 0)


def solution(mesh):
    return jax.shard_map(
        tile_gradient,
        mesh=mesh,
        in_specs=(
            P(None, None, "row", "col"),
            P(),
            P(),
            P("row", "col", None, None),
            P("row", "col"),
            P("row", "col", None, None, None),
        ),
        out_specs=P(None, None, "row", "col"),
        check_vma=False,
    )
```

```python
import functools
import math

import jax
import jax.numpy as jnp
import numpy as np
from jax import lax
from jax.experimental import pallas as pl
from jax.experimental.pallas import tpu as pltpu
from jax.sharding import PartitionSpec as P


floor_value = 0.1
lanes = 128


def shifted(block, axis, distance):
    devices = range(lax.axis_size(axis))
    route = [((i - distance) % len(devices), i) for i in devices]
    return lax.ppermute(block, axis, route)


def dft_tables(length):
    indices = np.arange(length, dtype=np.int32)
    turns = indices[:, None] * indices[None, :] % length
    angles = turns.astype(np.float32) * np.float32(2.0 * math.pi / length)
    cosine = np.cos(angles) / np.float32(math.sqrt(length))
    sine = np.sin(angles) / np.float32(math.sqrt(length))
    table_a = np.block([[cosine, sine], [-sine, cosine]])
    table_b = np.block([[cosine, -sine], [sine, cosine]])
    return (jnp.asarray(table_a, jnp.bfloat16), jnp.asarray(table_b, jnp.bfloat16))


def sections(stacked, left_table, right_table):
    length = stacked[0].shape[1]
    middle = [
        jnp.dot(left_table, wave, preferred_element_type=jnp.float32).astype(jnp.bfloat16)
        for wave in stacked
    ]
    middle = [jnp.concatenate([wave[:length], wave[length:]], 1) for wave in middle]
    result = [
        jnp.dot(wave, right_table, preferred_element_type=jnp.float32) for wave in middle
    ]
    return [(wave[:, :length], wave[:, length:]) for wave in result]


def transforms(waves, left_table, right_table):
    stacked = [
        jnp.concatenate([part.astype(jnp.bfloat16) for part in wave], 0) for wave in waves
    ]
    return sections(stacked, left_table, right_table)


def product_of(left, right):
    return left[0] * right[0] - left[1] * right[1], left[0] * right[1] + left[1] * right[0]


def conj_product(left, right):
    return left[0] * right[0] + left[1] * right[1], left[1] * right[0] - left[0] * right[1]


def strip_copies(array, strips, row0, store, plane, sem, outward):
    copies = []
    for s in range(array.shape[0]):
        for c in range(array.shape[1]):
            for k, strip in enumerate(strips):
                whole = array.at[s, c, :, pl.ds(k * lanes, lanes)]
                part = store.at[plane + s, c, strip, pl.ds(row0, array.shape[2]), :]
                source, target = (part, whole) if outward else (whole, part)
                copies.append(pltpu.make_async_copy(source, target, sem))
    return copies


def run_copies(groups):
    copies = [copy for group in groups for copy in group]
    for copy in copies:
        copy.start()
    return copies


def finish(copies):
    for copy in copies:
        copy.wait()


def patch_spot(places, slot):
    column = places[2 * slot + 1]
    return places[2 * slot], column // lanes, lax.rem(column, lanes)


def fetch(window, s, spot, length):
    row, strip, shift = spot
    back = lax.rem(lanes - shift, lanes)
    lane = lax.broadcasted_iota(jnp.int32, (length, lanes), 1)
    out = []
    for c in range(2):
        rolled = [
            pltpu.roll(window[s, c, strip + k, pl.ds(row, length), :], back, 1)
            for k in range(length // lanes + 1)
        ]
        parts = [
            jnp.where(lane < lanes - shift, rolled[k], rolled[k + 1])
            for k in range(length // lanes)
        ]
        out.append(jnp.concatenate(parts, 1))
    return tuple(out)


def accumulate(gradient, s, spot, wave, length):
    row, strip, shift = spot
    lane = lax.broadcasted_iota(jnp.int32, (length, lanes), 1)
    count = length // lanes
    for c in range(2):
        rolled = [
            pltpu.roll(wave[c][:, k * lanes : (k + 1) * lanes], shift, 1) for k in range(count)
        ]
        for k in range(count + 1):
            if k == 0:
                part = jnp.where(lane >= shift, rolled[0], 0.0)
            elif k == count:
                part = jnp.where(lane < shift, rolled[k - 1], 0.0)
            else:
                part = jnp.where(lane < shift, rolled[k - 1], rolled[k])
            at = (s, c, strip + k, pl.ds(row, length), slice(None))
            gradient[at] = gradient[at] + part


def spread_slots(places, window, constants, spreads, slots):
    probe, propagator, _, table_a, table_b = constants
    length = probe.shape[-1]
    waves = [
        product_of((probe[0], probe[1]), fetch(window, 0, patch_spot(places, slot), length))
        for slot in slots
    ]
    waves = transforms(waves, table_a[...], table_b[...])
    waves = [product_of((propagator[0], propagator[1]), wave) for wave in waves]
    waves = transforms(waves, table_b[...], table_a[...])
    for wave, slot in zip(waves, slots):
        spreads[slot, 0] = wave[0]
        spreads[slot, 1] = wave[1]


def back_slots(places, window, gradient, constants, spreads, inners, slots):
    probe, _, measured_ref, table_a, table_b = constants
    length = probe.shape[-1]
    spots = [patch_spot(places, slot) for slot in slots]
    waves = [
        product_of((spreads[slot, 0], spreads[slot, 1]), fetch(window, 1, spot, length))
        for slot, spot in zip(slots, spots)
    ]
    residuals = []
    for far, slot in zip(transforms(waves, table_a[...], table_b[...]), slots):
        power = far[0] * far[0] + far[1] * far[1]
        measured = measured_ref[slot].astype(jnp.float32)
        ratio = 1.0 - measured * jnp.minimum(lax.rsqrt(power), 1.0 / floor_value)
        residuals.append((far[0] * ratio, far[1] * ratio))
    backs = transforms(residuals, table_b[...], table_a[...])
    for back, slot, spot in zip(backs, slots, spots):
        inner = conj_product(back, fetch(window, 1, spot, length))
        inners[slot, pl.ds(0, length), :] = inner[0].astype(jnp.bfloat16)
        inners[slot, pl.ds(length, length), :] = inner[1].astype(jnp.bfloat16)
        spread = (spreads[slot, 0], spreads[slot, 1])
        accumulate(gradient, 1, spot, conj_product(back, spread), length)


def first_slots(places, gradient, constants, inners, slots):
    probe, propagator, _, table_a, table_b = constants
    length = probe.shape[-1]
    waves = sections([inners[slot] for slot in slots], table_a[...], table_b[...])
    waves = [conj_product(wave, (propagator[0], propagator[1])) for wave in waves]
    waves = transforms(waves, table_b[...], table_a[...])
    for wave, slot in zip(waves, slots):
        grad = conj_product(wave, (probe[0], probe[1]))
        accumulate(gradient, 0, patch_spot(places, slot), grad, length)


def visit_slots(places, count, slots, limit, inside, todo, exact, visit):
    def pick(slot, found):
        within = jnp.logical_and(places[2 * slot] <= limit, places[2 * slot + 1] <= limit)
        chosen = slot < count[0]
        if inside is not None:
            chosen = jnp.logical_and(chosen, within == inside)

        @pl.when(chosen)
        def _():
            todo[found] = slot

        return found + chosen.astype(jnp.int32)

    found = lax.fori_loop(0, slots, pick, jnp.int32(0))
    if exact:
        for size in range(1, slots + 1):

            @pl.when(found == size)
            def _():
                visit([todo[i] for i in range(size)])

        return

    def pair(index, carry):
        visit([todo[2 * index], todo[2 * index + 1]])
        return carry

    lax.fori_loop(0, found // 2, pair, 0)

    @pl.when(lax.rem(found, 2) == 1)
    def _():
        visit([todo[found - 1]])


def sizes(tile, length):
    own = range(tile // lanes)
    near = range(length // lanes)
    far = range(length // lanes, tile // lanes)
    past = range(tile // lanes, (tile + length) // lanes)
    return own, near, far, past


def from_strips(out, strips, row0, store, plane):
    for s in range(out.shape[0]):
        for c in range(out.shape[1]):
            for k, strip in enumerate(strips):
                out[s, c, :, pl.ds(k * lanes, lanes)] = store[
                    plane + s, c, strip, pl.ds(row0, out.shape[2]), :
                ]


def into_strips(piece, strips, row0, store, plane):
    for c in range(piece.shape[1]):
        for k, strip in enumerate(strips):
            store[plane, c, strip, pl.ds(row0, piece.shape[2]), :] = piece[
                0, c, :, pl.ds(k * lanes, lanes)
            ]


def pack_kernel(corners, object_ref, *rest):
    outs, sem = rest[:-1], rest[-1]
    copies = []
    for (s, row, column), out in zip(corners, outs):
        for c in range(out.shape[1]):
            piece = object_ref.at[
                s, c, pl.ds(row, out.shape[2]), pl.ds(column, out.shape[3])
            ]
            copies.append(pltpu.make_async_copy(piece, out.at[0, c], sem))
    for copy in copies:
        copy.start()
    finish(copies)


def pack(object_field, pieces):
    return pl.pallas_call(
        functools.partial(pack_kernel, [piece[:3] for piece in pieces]),
        out_shape=[
            pltpu.VMEM((1, object_field.shape[1], *piece[3:]), jnp.float32)
            for piece in pieces
        ],
        in_specs=[hbm_space],
        out_specs=[vmem_space] * len(pieces),
        scratch_shapes=[pltpu.SemaphoreType.DMA],
        compiler_params=pltpu.CompilerParams(vmem_limit_bytes=6 * 1024 * 1024),
    )(in_hbm(object_field))


def own_slots_kernel(places, count, object_ref, *rest):
    constants, (window, gradient, spreads, inners, todo, sem) = rest[:5], rest[5:]
    length = constants[0].shape[-1]
    tile = object_ref.shape[-1]
    own, _, _, _ = sizes(tile, length)
    loads = run_copies([strip_copies(object_ref, own, 0, window, 0, sem, False)])
    gradient[...] = jnp.zeros_like(gradient)
    finish(loads)

    def visit(slots):
        spread_slots(places, window, constants, spreads, slots)
        back_slots(places, window, gradient, constants, spreads, inners, slots)

    visit_slots(
        places, count, inners.shape[0], tile - length, True, todo, False, visit
    )


def spread_kernel(places, count, near_ref, far_ref, corner_ref, right_ref, *rest):
    constants, (window, gradient, spreads, inners, todo, sem) = rest[:5], rest[9:]
    length = constants[0].shape[-1]
    tile = right_ref.shape[2]
    _, near, far, past = sizes(tile, length)
    finish(
        run_copies(
            [
                strip_copies(near_ref, near, tile, window, 0, sem, False),
                strip_copies(far_ref, far, tile, window, 0, sem, False),
                strip_copies(corner_ref, past, tile, window, 0, sem, False),
                strip_copies(right_ref, past, 0, window, 0, sem, False),
            ]
        )
    )

    def visit(slots):
        spread_slots(places, window, constants, spreads, slots)

    visit_slots(
        places, count, inners.shape[0], tile - length, False, todo, False, visit
    )


def load_kernel(near_ref, corner_ref, right_ref, window_in, window, sem):
    del window_in
    length = near_ref.shape[3]
    tile = right_ref.shape[2]
    _, near, _, past = sizes(tile, length)
    finish(
        run_copies(
            [
                strip_copies(near_ref, near, tile, window, 1, sem, False),
                strip_copies(corner_ref, past, tile, window, 1, sem, False),
                strip_copies(right_ref, past, 0, window, 1, sem, False),
            ]
        )
    )


def back_kernel(places, count, far_ref, *rest):
    constants = rest[:5]
    near_out, far_out, corner_out, window, gradient, spreads, inners, todo, _ = rest[9:]
    length = constants[0].shape[-1]
    tile = length + far_ref.shape[3]
    _, near, far, past = sizes(tile, length)
    into_strips(far_ref, far, tile, window, 1)

    def visit(slots):
        back_slots(places, window, gradient, constants, spreads, inners, slots)

    visit_slots(
        places, count, inners.shape[0], tile - length, False, todo, True, visit
    )
    from_strips(corner_out, past, tile, gradient, 1)
    from_strips(far_out, far, tile, gradient, 1)
    from_strips(near_out, near, tile, gradient, 1)


def first_kernel(places, count, *rest):
    constants = rest[:5]
    near_out, far_out, corner_out, right_out = rest[9:13]
    _, gradient, _, inners, todo, _ = rest[13:]
    length = constants[0].shape[-1]
    tile = length + far_out.shape[3]
    _, near, far, past = sizes(tile, length)

    def visit(slots):
        first_slots(places, gradient, constants, inners, slots)

    visit_slots(
        places, count, inners.shape[0], tile - length, None, todo, False, visit
    )
    from_strips(corner_out, past, tile, gradient, 0)
    from_strips(far_out, far, tile, gradient, 0)
    from_strips(near_out, near, tile, gradient, 0)
    from_strips(right_out, past, 0, gradient, 0)


def own_kernel(gradient, own_out, sem):
    tile = own_out.shape[-1]
    finish(run_copies([strip_copies(own_out, range(tile // lanes), 0, gradient, 0, sem, True)]))


def add_kernel(plane, column, gradient_in, piece_ref, gradient_out, held, added, sems):
    del gradient_in
    slices, parts, rows, columns = piece_ref.shape
    planes = [(s, c) for s in range(slices) for c in range(parts)]

    def spot(s, c):
        return gradient_out.at[plane + s, c, pl.ds(0, rows), pl.ds(column, columns)]

    loads, pieces, stores = [], [], []
    for i, (s, c) in enumerate(planes):
        loads.append(pltpu.make_async_copy(spot(s, c), held.at[i], sems.at[0, i]))
        pieces.append(pltpu.make_async_copy(piece_ref.at[s, c], added.at[i], sems.at[1, i]))
        stores.append(pltpu.make_async_copy(held.at[i], spot(s, c), sems.at[2, i]))
        loads[i].start()
        pieces[i].start()
    for i in range(len(planes)):
        loads[i].wait()
        pieces[i].wait()
        held[i] = held[i] + added[i]
        stores[i].start()
    finish(stores)


def add_piece(gradient, piece, plane, column):
    slices, parts, rows, columns = piece.shape
    planes = slices * parts
    return pl.pallas_call(
        functools.partial(add_kernel, plane, column),
        out_shape=jax.ShapeDtypeStruct(gradient.shape, gradient.dtype),
        in_specs=[any_space] * 2,
        out_specs=any_space,
        scratch_shapes=[pltpu.VMEM((planes, rows, columns), jnp.float32)] * 2
        + [pltpu.SemaphoreType.DMA((3, planes))],
        input_output_aliases={0: 0},
        compiler_params=pltpu.CompilerParams(vmem_limit_bytes=8 * 1024 * 1024),
    )(gradient, piece)


def corner_copies(gradient, held, sem, outward):
    copies = []
    for c in range(held.shape[1]):
        part = gradient.at[0, c, pl.ds(0, held.shape[2]), pl.ds(0, held.shape[3])]
        source, target = (held.at[0, c], part) if outward else (part, held.at[0, c])
        copies.append(pltpu.make_async_copy(source, target, sem))
    return copies


def hold_kernel(gradient, held, sem):
    finish(run_copies([corner_copies(gradient, held, sem, False)]))


def last_kernel(gradient_in, held, piece, gradient, total, sem):
    del gradient_in
    stores = corner_copies(gradient, total, sem, True)
    for c, store in enumerate(stores):
        total[0, c] = held[0, c] + piece[0, c]
        store.start()
    finish(stores)


def in_hbm(x):
    return pltpu.with_memory_space_constraint(x, pltpu.HBM)


def in_vmem(x):
    return pltpu.with_memory_space_constraint(x, pltpu.VMEM)


any_space = pl.BlockSpec(memory_space=pl.ANY)
hbm_space = pl.BlockSpec(memory_space=pltpu.HBM)
vmem_space = pl.BlockSpec(memory_space=pltpu.VMEM)
scalar_space = pl.BlockSpec(memory_space=pltpu.SMEM)


def slots_call(body, scalars, pieces, constants, state, state_types, out_shapes):
    first = len(scalars) + len(pieces) + len(constants)
    aliases = {first + i: len(out_shapes) + i for i in range(len(state))}
    close = bool(out_shapes)
    if close:
        pieces = [in_vmem(piece) for piece in pieces]
    piece_space = vmem_space if close else any_space if state else hbm_space
    return pl.pallas_call(
        body,
        out_shape=[pltpu.VMEM(s, jnp.float32) for s in out_shapes] + state_types,
        in_specs=[scalar_space] * len(scalars)
        + [piece_space] * len(pieces)
        + [vmem_space] * (len(constants) + len(state)),
        out_specs=[vmem_space] * (len(out_shapes) + len(state_types)),
        scratch_shapes=[
            pltpu.SMEM((constants[2].shape[0],), jnp.int32),
            pltpu.SemaphoreType.DMA,
        ],
        input_output_aliases=aliases,
        compiler_params=pltpu.CompilerParams(vmem_limit_bytes=20 * 1024 * 1024),
    )(*scalars, *pieces, *[in_vmem(x) for x in (*constants, *state)])


def tile_gradient(object_field, probe_field, propagator_phase, positions, counts, amplitudes):
    length = probe_field.shape[-1]
    tile = object_field.shape[-1]
    slices, parts = object_field.shape[:2]
    slots = positions.shape[-2]

    rest = tile - length
    (near0,) = pack(object_field, [(0, 0, 0, length, length)])
    right0, far0, near1, far1, right1 = pack(
        object_field,
        [
            (0, 0, 0, tile, length),
            (0, 0, length, length, rest),
            (1, 0, 0, length, length),
            (1, 0, length, length, rest),
            (1, 0, 0, tile, length),
        ],
    )
    near0 = shifted(near0, "row", -1)
    right0 = shifted(right0, "col", -1)
    far0 = shifted(far0, "row", -1)
    near1 = shifted(near1, "row", -1)
    far1 = shifted(far1, "row", -1)
    right1 = shifted(right1, "col", -1)
    corner0 = shifted(near0, "col", -1)
    corner1 = shifted(near1, "col", -1)

    propagator = jnp.stack([jnp.cos(propagator_phase), jnp.sin(propagator_phase)], 0)
    constants = (probe_field, propagator, amplitudes[0, 0], *dft_tables(length))
    scalars = (positions.reshape(-1), counts.reshape(-1))
    strips = (slices, parts, (tile + length) // lanes, tile + length, lanes)
    state_types = [
        pltpu.VMEM(strips, jnp.float32),
        pltpu.VMEM(strips, jnp.float32),
        pltpu.VMEM((slots, parts, length, length), jnp.float32),
        pltpu.VMEM((slots, parts * length, length), jnp.bfloat16),
    ]
    piece_shapes = (
        (1, parts, length, length),
        (1, parts, length, tile - length),
        (1, parts, length, length),
    )

    def call(kernel, pieces, state, out_shapes):
        return slots_call(kernel, scalars, pieces, constants, state, state_types, out_shapes)

    state = call(own_slots_kernel, (in_hbm(object_field),), (), ())
    state = call(spread_kernel, (near0, far0, corner0, right0), state, ())
    window, *others = state
    window = pl.pallas_call(
        load_kernel,
        name="load_halo",
        out_shape=state_types[0],
        in_specs=[any_space] * 3 + [vmem_space],
        out_specs=vmem_space,
        scratch_shapes=[pltpu.SemaphoreType.DMA],
        input_output_aliases={3: 0},
        compiler_params=pltpu.CompilerParams(vmem_limit_bytes=4 * 1024 * 1024),
    )(near1, corner1, right1, in_vmem(window))
    near1, far1, corner1, *state = call(back_kernel, (far1,), (window, *others), piece_shapes)
    corner1 = shifted(corner1, "col", 1)
    far1 = shifted(far1, "row", 1)
    near0, far0, corner0, right, window, gradient, *_ = call(
        first_kernel, (), state, (*piece_shapes, (slices, parts, tile, length))
    )
    near1 = shifted(near1 + corner1, "row", 1)
    corner0 = shifted(corner0, "col", 1)
    right = shifted(right, "col", 1)
    far0 = shifted(far0, "row", 1)
    own = pl.pallas_call(
        own_kernel,
        name="own",
        out_shape=jax.ShapeDtypeStruct(object_field.shape, jnp.float32),
        in_specs=[vmem_space],
        out_specs=any_space,
        scratch_shapes=[pltpu.SemaphoreType.DMA],
        compiler_params=pltpu.CompilerParams(vmem_limit_bytes=1024 * 1024),
    )(in_vmem(gradient))
    near0 = shifted(near0 + corner0, "row", 1)
    result = add_piece(own, far1, 1, length)
    result = add_piece(result, near1, 1, 0)
    result = add_piece(result, right, 0, 0)
    result = add_piece(result, far0, 0, length)
    held = pl.pallas_call(
        hold_kernel,
        name="hold",
        out_shape=pltpu.VMEM(near0.shape, jnp.float32),
        in_specs=[any_space],
        out_specs=vmem_space,
        scratch_shapes=[pltpu.SemaphoreType.DMA],
        compiler_params=pltpu.CompilerParams(vmem_limit_bytes=2 * 1024 * 1024),
    )(in_hbm(result))
    return pl.pallas_call(
        last_kernel,
        name="add_near0",
        out_shape=jax.ShapeDtypeStruct(result.shape, jnp.float32),
        in_specs=[any_space, vmem_space, vmem_space],
        out_specs=any_space,
        scratch_shapes=[pltpu.VMEM(near0.shape, jnp.float32), pltpu.SemaphoreType.DMA],
        input_output_aliases={0: 0},
        compiler_params=pltpu.CompilerParams(vmem_limit_bytes=2 * 1024 * 1024),
    )(result, in_vmem(held), in_vmem(near0))


def solution(mesh):
    return jax.shard_map(
        tile_gradient,
        mesh=mesh,
        in_specs=(
            P(None, None, "row", "col"),
            P(),
            P(),
            P("row", "col", None, None),
            P("row", "col"),
            P("row", "col", None, None, None),
        ),
        out_specs=P(None, None, "row", "col"),
        check_vma=False,
    )
```

```python
import functools
import math

import jax
import jax.numpy as jnp
import numpy as np
from jax import lax
from jax.experimental import pallas as pl
from jax.experimental.pallas import tpu as pltpu
from jax.sharding import PartitionSpec as P


floor_value = 0.1
lanes = 128


def shifted(block, axis, distance):
    devices = range(lax.axis_size(axis))
    route = [((i - distance) % len(devices), i) for i in devices]
    return lax.ppermute(block, axis, route)


def dft_tables(length):
    indices = np.arange(length, dtype=np.int32)
    turns = indices[:, None] * indices[None, :] % length
    angles = turns.astype(np.float32) * np.float32(2.0 * math.pi / length)
    cosine = np.cos(angles) / np.float32(math.sqrt(length))
    sine = np.sin(angles) / np.float32(math.sqrt(length))
    table_a = np.block([[cosine, sine], [-sine, cosine]])
    table_b = np.block([[cosine, -sine], [sine, cosine]])
    return (jnp.asarray(table_a, jnp.bfloat16), jnp.asarray(table_b, jnp.bfloat16))


def sections(stacked, left_table, right_table):
    length = stacked[0].shape[1]
    middle = [
        jnp.dot(left_table, wave, preferred_element_type=jnp.float32).astype(jnp.bfloat16)
        for wave in stacked
    ]
    middle = [jnp.concatenate([wave[:length], wave[length:]], 1) for wave in middle]
    result = [
        jnp.dot(wave, right_table, preferred_element_type=jnp.float32) for wave in middle
    ]
    return [(wave[:, :length], wave[:, length:]) for wave in result]


def transforms(waves, left_table, right_table):
    stacked = [
        jnp.concatenate([part.astype(jnp.bfloat16) for part in wave], 0) for wave in waves
    ]
    return sections(stacked, left_table, right_table)


def product_of(left, right):
    return left[0] * right[0] - left[1] * right[1], left[0] * right[1] + left[1] * right[0]


def conj_product(left, right):
    return left[0] * right[0] + left[1] * right[1], left[1] * right[0] - left[0] * right[1]


def strip_copies(array, strips, row0, store, plane, sem, outward):
    copies = []
    for s in range(array.shape[0]):
        for c in range(array.shape[1]):
            for k, strip in enumerate(strips):
                whole = array.at[s, c, :, pl.ds(k * lanes, lanes)]
                part = store.at[plane + s, c, strip, pl.ds(row0, array.shape[2]), :]
                source, target = (part, whole) if outward else (whole, part)
                copies.append(pltpu.make_async_copy(source, target, sem))
    return copies


def run_copies(groups):
    copies = [copy for group in groups for copy in group]
    for copy in copies:
        copy.start()
    return copies


def finish(copies):
    for copy in copies:
        copy.wait()


def patch_spot(places, slot):
    column = places[2 * slot + 1]
    return places[2 * slot], column // lanes, lax.rem(column, lanes)


def fetch(window, s, spot, length):
    row, strip, shift = spot
    back = lax.rem(lanes - shift, lanes)
    lane = lax.broadcasted_iota(jnp.int32, (length, lanes), 1)
    out = []
    for c in range(2):
        rolled = [
            pltpu.roll(window[s, c, strip + k, pl.ds(row, length), :], back, 1)
            for k in range(length // lanes + 1)
        ]
        parts = [
            jnp.where(lane < lanes - shift, rolled[k], rolled[k + 1])
            for k in range(length // lanes)
        ]
        out.append(jnp.concatenate(parts, 1))
    return tuple(out)


def accumulate(gradient, s, spot, wave, length):
    row, strip, shift = spot
    lane = lax.broadcasted_iota(jnp.int32, (length, lanes), 1)
    count = length // lanes
    for c in range(2):
        rolled = [
            pltpu.roll(wave[c][:, k * lanes : (k + 1) * lanes], shift, 1) for k in range(count)
        ]
        for k in range(count + 1):
            if k == 0:
                part = jnp.where(lane >= shift, rolled[0], 0.0)
            elif k == count:
                part = jnp.where(lane < shift, rolled[k - 1], 0.0)
            else:
                part = jnp.where(lane < shift, rolled[k - 1], rolled[k])
            at = (s, c, strip + k, pl.ds(row, length), slice(None))
            gradient[at] = gradient[at] + part


def spread_slots(places, window, constants, spreads, slots):
    probe, propagator, _, table_a, table_b = constants
    length = probe.shape[-1]
    waves = [
        product_of((probe[0], probe[1]), fetch(window, 0, patch_spot(places, slot), length))
        for slot in slots
    ]
    waves = transforms(waves, table_a[...], table_b[...])
    waves = [product_of((propagator[0], propagator[1]), wave) for wave in waves]
    waves = transforms(waves, table_b[...], table_a[...])
    for wave, slot in zip(waves, slots):
        spreads[slot, 0] = wave[0]
        spreads[slot, 1] = wave[1]


def back_slots(places, window, gradient, constants, spreads, inners, slots):
    probe, _, measured_ref, table_a, table_b = constants
    length = probe.shape[-1]
    spots = [patch_spot(places, slot) for slot in slots]
    waves = [
        product_of((spreads[slot, 0], spreads[slot, 1]), fetch(window, 1, spot, length))
        for slot, spot in zip(slots, spots)
    ]
    residuals = []
    for far, slot in zip(transforms(waves, table_a[...], table_b[...]), slots):
        power = far[0] * far[0] + far[1] * far[1]
        measured = measured_ref[slot].astype(jnp.float32)
        ratio = 1.0 - measured * jnp.minimum(lax.rsqrt(power), 1.0 / floor_value)
        residuals.append((far[0] * ratio, far[1] * ratio))
    backs = transforms(residuals, table_b[...], table_a[...])
    for back, slot, spot in zip(backs, slots, spots):
        inner = conj_product(back, fetch(window, 1, spot, length))
        inners[slot, pl.ds(0, length), :] = inner[0].astype(jnp.bfloat16)
        inners[slot, pl.ds(length, length), :] = inner[1].astype(jnp.bfloat16)
        spread = (spreads[slot, 0], spreads[slot, 1])
        accumulate(gradient, 1, spot, conj_product(back, spread), length)


def first_slots(places, gradient, constants, inners, slots):
    probe, propagator, _, table_a, table_b = constants
    length = probe.shape[-1]
    waves = sections([inners[slot] for slot in slots], table_a[...], table_b[...])
    waves = [conj_product(wave, (propagator[0], propagator[1])) for wave in waves]
    waves = transforms(waves, table_b[...], table_a[...])
    for wave, slot in zip(waves, slots):
        grad = conj_product(wave, (probe[0], probe[1]))
        accumulate(gradient, 0, patch_spot(places, slot), grad, length)


def visit_slots(places, count, slots, limit, inside, todo, exact, visit):
    def pick(slot, found):
        within = jnp.logical_and(places[2 * slot] <= limit, places[2 * slot + 1] <= limit)
        chosen = slot < count[0]
        if inside is not None:
            chosen = jnp.logical_and(chosen, within == inside)

        @pl.when(chosen)
        def _():
            todo[found] = slot

        return found + chosen.astype(jnp.int32)

    found = lax.fori_loop(0, slots, pick, jnp.int32(0))
    if exact:
        for size in range(1, slots + 1):

            @pl.when(found == size)
            def _():
                visit([todo[i] for i in range(size)])

        return

    def pair(index, carry):
        visit([todo[2 * index], todo[2 * index + 1]])
        return carry

    lax.fori_loop(0, found // 2, pair, 0)

    @pl.when(lax.rem(found, 2) == 1)
    def _():
        visit([todo[found - 1]])


def sizes(tile, length):
    own = range(tile // lanes)
    near = range(length // lanes)
    far = range(length // lanes, tile // lanes)
    past = range(tile // lanes, (tile + length) // lanes)
    return own, near, far, past


def from_strips(out, strips, row0, store, plane):
    for s in range(out.shape[0]):
        for c in range(out.shape[1]):
            for k, strip in enumerate(strips):
                out[s, c, :, pl.ds(k * lanes, lanes)] = store[
                    plane + s, c, strip, pl.ds(row0, out.shape[2]), :
                ]


def into_strips(piece, strips, row0, store, plane):
    for c in range(piece.shape[1]):
        for k, strip in enumerate(strips):
            store[plane, c, strip, pl.ds(row0, piece.shape[2]), :] = piece[
                0, c, :, pl.ds(k * lanes, lanes)
            ]


def pack_near_kernel(object_ref, start, out, sem):
    del start
    finish(run_copies([corner_copies(object_ref, out, sem, False)]))


def pack_kernel(corners, object_ref, *rest):
    outs, sem = rest[:-1], rest[-1]
    copies = []
    for (s, row, column), out in zip(corners, outs):
        for c in range(out.shape[1]):
            piece = object_ref.at[
                s, c, pl.ds(row, out.shape[2]), pl.ds(column, out.shape[3])
            ]
            copies.append(pltpu.make_async_copy(piece, out.at[0, c], sem))
    for copy in copies:
        copy.start()
    finish(copies)


def pack(object_field, pieces):
    return pl.pallas_call(
        functools.partial(pack_kernel, [piece[:3] for piece in pieces]),
        out_shape=[
            pltpu.VMEM((1, object_field.shape[1], *piece[3:]), jnp.float32)
            for piece in pieces
        ],
        in_specs=[hbm_space],
        out_specs=[vmem_space] * len(pieces),
        scratch_shapes=[pltpu.SemaphoreType.DMA],
        compiler_params=pltpu.CompilerParams(vmem_limit_bytes=6 * 1024 * 1024),
    )(in_hbm(object_field))


def own_slots_kernel(places, count, object_ref, *rest):
    constants, (window, gradient, spreads, inners, todo, sem) = rest[:5], rest[5:]
    length = constants[0].shape[-1]
    tile = object_ref.shape[-1]
    own, _, _, _ = sizes(tile, length)
    loads = run_copies([strip_copies(object_ref, own, 0, window, 0, sem, False)])
    gradient[...] = jnp.zeros_like(gradient)
    finish(loads)

    def visit(slots):
        spread_slots(places, window, constants, spreads, slots)
        back_slots(places, window, gradient, constants, spreads, inners, slots)

    visit_slots(
        places, count, inners.shape[0], tile - length, True, todo, False, visit
    )


def spread_kernel(places, count, near_ref, far_ref, corner_ref, right_ref, *rest):
    constants, (window, gradient, spreads, inners, todo, sem) = rest[:5], rest[9:]
    length = constants[0].shape[-1]
    tile = right_ref.shape[2]
    _, near, far, past = sizes(tile, length)
    finish(
        run_copies(
            [
                strip_copies(near_ref, near, tile, window, 0, sem, False),
                strip_copies(far_ref, far, tile, window, 0, sem, False),
                strip_copies(corner_ref, past, tile, window, 0, sem, False),
                strip_copies(right_ref, past, 0, window, 0, sem, False),
            ]
        )
    )

    def visit(slots):
        spread_slots(places, window, constants, spreads, slots)

    visit_slots(
        places, count, inners.shape[0], tile - length, False, todo, False, visit
    )


def load_kernel(near_ref, corner_ref, right_ref, window_in, window, sem):
    del window_in
    length = near_ref.shape[3]
    tile = right_ref.shape[2]
    _, near, _, past = sizes(tile, length)
    finish(
        run_copies(
            [
                strip_copies(near_ref, near, tile, window, 1, sem, False),
                strip_copies(corner_ref, past, tile, window, 1, sem, False),
                strip_copies(right_ref, past, 0, window, 1, sem, False),
            ]
        )
    )


def back_kernel(places, count, far_ref, *rest):
    constants = rest[:5]
    near_out, far_out, corner_out, window, gradient, spreads, inners, todo, _ = rest[9:]
    length = constants[0].shape[-1]
    tile = length + far_ref.shape[3]
    _, near, far, past = sizes(tile, length)
    into_strips(far_ref, far, tile, window, 1)

    def visit(slots):
        back_slots(places, window, gradient, constants, spreads, inners, slots)

    visit_slots(
        places, count, inners.shape[0], tile - length, False, todo, True, visit
    )
    from_strips(corner_out, past, tile, gradient, 1)
    from_strips(far_out, far, tile, gradient, 1)
    from_strips(near_out, near, tile, gradient, 1)


def first_kernel(places, count, *rest):
    constants = rest[:5]
    near_out, far_out, corner_out, right_out = rest[9:13]
    _, gradient, _, inners, todo, _ = rest[13:]
    length = constants[0].shape[-1]
    tile = length + far_out.shape[3]
    _, near, far, past = sizes(tile, length)

    def visit(slots):
        first_slots(places, gradient, constants, inners, slots)

    visit_slots(
        places, count, inners.shape[0], tile - length, None, todo, False, visit
    )
    from_strips(corner_out, past, tile, gradient, 0)
    from_strips(far_out, far, tile, gradient, 0)
    from_strips(near_out, near, tile, gradient, 0)
    from_strips(right_out, past, 0, gradient, 0)


def own_kernel(gradient, own_out, sem):
    tile = own_out.shape[-1]
    finish(run_copies([strip_copies(own_out, range(tile // lanes), 0, gradient, 0, sem, True)]))


def add_kernel(plane, column, gradient_in, piece_ref, gradient_out, held, added, sems):
    del gradient_in
    slices, parts, rows, columns = piece_ref.shape
    planes = [(s, c) for s in range(slices) for c in range(parts)]

    def spot(s, c):
        return gradient_out.at[plane + s, c, pl.ds(0, rows), pl.ds(column, columns)]

    loads, pieces, stores = [], [], []
    for i, (s, c) in enumerate(planes):
        loads.append(pltpu.make_async_copy(spot(s, c), held.at[i], sems.at[0, i]))
        pieces.append(pltpu.make_async_copy(piece_ref.at[s, c], added.at[i], sems.at[1, i]))
        stores.append(pltpu.make_async_copy(held.at[i], spot(s, c), sems.at[2, i]))
        loads[i].start()
        pieces[i].start()
    for i in range(len(planes)):
        loads[i].wait()
        pieces[i].wait()
        held[i] = held[i] + added[i]
        stores[i].start()
    finish(stores)


def add_piece(gradient, piece, plane, column):
    slices, parts, rows, columns = piece.shape
    planes = slices * parts
    return pl.pallas_call(
        functools.partial(add_kernel, plane, column),
        out_shape=jax.ShapeDtypeStruct(gradient.shape, gradient.dtype),
        in_specs=[any_space] * 2,
        out_specs=any_space,
        scratch_shapes=[pltpu.VMEM((planes, rows, columns), jnp.float32)] * 2
        + [pltpu.SemaphoreType.DMA((3, planes))],
        input_output_aliases={0: 0},
        compiler_params=pltpu.CompilerParams(vmem_limit_bytes=8 * 1024 * 1024),
    )(gradient, piece)


def corner_copies(gradient, held, sem, outward):
    copies = []
    for c in range(held.shape[1]):
        part = gradient.at[0, c, pl.ds(0, held.shape[2]), pl.ds(0, held.shape[3])]
        source, target = (held.at[0, c], part) if outward else (part, held.at[0, c])
        copies.append(pltpu.make_async_copy(source, target, sem))
    return copies


def hold_kernel(gradient, held, sem):
    finish(run_copies([corner_copies(gradient, held, sem, False)]))


def last_kernel(gradient_in, held, piece, gradient, total, sem):
    del gradient_in
    stores = corner_copies(gradient, total, sem, True)
    for c, store in enumerate(stores):
        total[0, c] = held[0, c] + piece[0, c]
        store.start()
    finish(stores)


def in_hbm(x):
    return pltpu.with_memory_space_constraint(x, pltpu.HBM)


def in_vmem(x):
    return pltpu.with_memory_space_constraint(x, pltpu.VMEM)


any_space = pl.BlockSpec(memory_space=pl.ANY)
hbm_space = pl.BlockSpec(memory_space=pltpu.HBM)
vmem_space = pl.BlockSpec(memory_space=pltpu.VMEM)
scalar_space = pl.BlockSpec(memory_space=pltpu.SMEM)


def slots_call(body, scalars, pieces, constants, state, state_types, out_shapes):
    first = len(scalars) + len(pieces) + len(constants)
    aliases = {first + i: len(out_shapes) + i for i in range(len(state))}
    close = bool(out_shapes)
    if close:
        pieces = [in_vmem(piece) for piece in pieces]
    piece_space = vmem_space if close else any_space if state else hbm_space
    return pl.pallas_call(
        body,
        out_shape=[pltpu.VMEM(s, jnp.float32) for s in out_shapes] + state_types,
        in_specs=[scalar_space] * len(scalars)
        + [piece_space] * len(pieces)
        + [vmem_space] * (len(constants) + len(state)),
        out_specs=[vmem_space] * (len(out_shapes) + len(state_types)),
        scratch_shapes=[
            pltpu.SMEM((constants[2].shape[0],), jnp.int32),
            pltpu.SemaphoreType.DMA,
        ],
        input_output_aliases=aliases,
        compiler_params=pltpu.CompilerParams(vmem_limit_bytes=20 * 1024 * 1024),
    )(*scalars, *pieces, *[in_vmem(x) for x in (*constants, *state)])


def tile_gradient(object_field, probe_field, propagator_phase, positions, counts, amplitudes):
    length = probe_field.shape[-1]
    tile = object_field.shape[-1]
    slices, parts = object_field.shape[:2]
    slots = positions.shape[-2]

    rest = tile - length
    near0 = pl.pallas_call(
        pack_near_kernel,
        name="pack0",
        out_shape=pltpu.VMEM((1, parts, length, length), jnp.float32),
        in_specs=[hbm_space, vmem_space],
        out_specs=vmem_space,
        scratch_shapes=[pltpu.SemaphoreType.DMA],
        input_output_aliases={1: 0},
        compiler_params=pltpu.CompilerParams(vmem_limit_bytes=1024 * 1024),
    )(in_hbm(object_field), in_vmem(jnp.zeros((1, parts, length, length), jnp.float32)))
    right0, far0, near1, far1, right1 = pack(
        object_field,
        [
            (0, 0, 0, tile, length),
            (0, 0, length, length, rest),
            (1, 0, 0, length, length),
            (1, 0, length, length, rest),
            (1, 0, 0, tile, length),
        ],
    )
    near0 = shifted(near0, "row", -1)
    right0 = shifted(right0, "col", -1)
    far0 = shifted(far0, "row", -1)
    near1 = shifted(near1, "row", -1)
    far1 = shifted(far1, "row", -1)
    right1 = shifted(right1, "col", -1)
    corner0 = shifted(near0, "col", -1)
    corner1 = shifted(near1, "col", -1)

    propagator = jnp.stack([jnp.cos(propagator_phase), jnp.sin(propagator_phase)], 0)
    constants = (probe_field, propagator, amplitudes[0, 0], *dft_tables(length))
    scalars = (positions.reshape(-1), counts.reshape(-1))
    strips = (slices, parts, (tile + length) // lanes, tile + length, lanes)
    state_types = [
        pltpu.VMEM(strips, jnp.float32),
        pltpu.VMEM(strips, jnp.float32),
        pltpu.VMEM((slots, parts, length, length), jnp.float32),
        pltpu.VMEM((slots, parts * length, length), jnp.bfloat16),
    ]
    piece_shapes = (
        (1, parts, length, length),
        (1, parts, length, tile - length),
        (1, parts, length, length),
    )

    def call(kernel, pieces, state, out_shapes):
        return slots_call(kernel, scalars, pieces, constants, state, state_types, out_shapes)

    state = call(own_slots_kernel, (in_hbm(object_field),), (), ())
    state = call(spread_kernel, (near0, far0, corner0, right0), state, ())
    window, *others = state
    window = pl.pallas_call(
        load_kernel,
        name="load",
        out_shape=state_types[0],
        in_specs=[any_space] * 3 + [vmem_space],
        out_specs=vmem_space,
        scratch_shapes=[pltpu.SemaphoreType.DMA],
        input_output_aliases={3: 0},
        compiler_params=pltpu.CompilerParams(vmem_limit_bytes=4 * 1024 * 1024),
    )(near1, corner1, right1, in_vmem(window))
    near1, far1, corner1, *state = call(back_kernel, (far1,), (window, *others), piece_shapes)
    corner1 = shifted(corner1, "col", 1)
    far1 = shifted(far1, "row", 1)
    near0, far0, corner0, right, window, gradient, *_ = call(
        first_kernel, (), state, (*piece_shapes, (slices, parts, tile, length))
    )
    near1 = shifted(near1 + corner1, "row", 1)
    corner0 = shifted(corner0, "col", 1)
    right = shifted(right, "col", 1)
    far0 = shifted(far0, "row", 1)
    own = pl.pallas_call(
        own_kernel,
        name="store",
        out_shape=jax.ShapeDtypeStruct(object_field.shape, jnp.float32),
        in_specs=[vmem_space],
        out_specs=any_space,
        scratch_shapes=[pltpu.SemaphoreType.DMA],
        compiler_params=pltpu.CompilerParams(vmem_limit_bytes=1024 * 1024),
    )(in_vmem(gradient))
    near0 = shifted(near0 + corner0, "row", 1)
    result = add_piece(own, far1, 1, length)
    result = add_piece(result, near1, 1, 0)
    result = add_piece(result, right, 0, 0)
    result = add_piece(result, far0, 0, length)
    held = pl.pallas_call(
        hold_kernel,
        name="hold",
        out_shape=pltpu.VMEM(near0.shape, jnp.float32),
        in_specs=[any_space],
        out_specs=vmem_space,
        scratch_shapes=[pltpu.SemaphoreType.DMA],
        compiler_params=pltpu.CompilerParams(vmem_limit_bytes=2 * 1024 * 1024),
    )(in_hbm(result))
    return pl.pallas_call(
        last_kernel,
        name="addn0",
        out_shape=jax.ShapeDtypeStruct(result.shape, jnp.float32),
        in_specs=[any_space, vmem_space, vmem_space],
        out_specs=any_space,
        scratch_shapes=[pltpu.VMEM(near0.shape, jnp.float32), pltpu.SemaphoreType.DMA],
        input_output_aliases={0: 0},
        compiler_params=pltpu.CompilerParams(vmem_limit_bytes=2 * 1024 * 1024),
    )(result, in_vmem(held), in_vmem(near0))


def solution(mesh):
    return jax.shard_map(
        tile_gradient,
        mesh=mesh,
        in_specs=(
            P(None, None, "row", "col"),
            P(),
            P(),
            P("row", "col", None, None),
            P("row", "col"),
            P("row", "col", None, None, None),
        ),
        out_specs=P(None, None, "row", "col"),
        check_vma=False,
    )
```

```python
import functools
import math

import jax
import jax.numpy as jnp
import numpy as np
from jax import lax
from jax.experimental import pallas as pl
from jax.experimental.pallas import tpu as pltpu
from jax.sharding import PartitionSpec as P


floor_value = 0.1
lanes = 128


def shifted(block, axis, distance):
    devices = range(lax.axis_size(axis))
    route = [((i - distance) % len(devices), i) for i in devices]
    return lax.ppermute(block, axis, route)


def dft_tables(length):
    indices = np.arange(length, dtype=np.int32)
    turns = indices[:, None] * indices[None, :] % length
    angles = turns.astype(np.float32) * np.float32(2.0 * math.pi / length)
    cosine = np.cos(angles) / np.float32(math.sqrt(length))
    sine = np.sin(angles) / np.float32(math.sqrt(length))
    table_a = np.block([[cosine, sine], [-sine, cosine]])
    table_b = np.block([[cosine, -sine], [sine, cosine]])
    return (jnp.asarray(table_a, jnp.bfloat16), jnp.asarray(table_b, jnp.bfloat16))


def sections(stacked, left_table, right_table):
    length = stacked[0].shape[1]
    middle = [
        jnp.dot(left_table, wave, preferred_element_type=jnp.float32).astype(jnp.bfloat16)
        for wave in stacked
    ]
    middle = [jnp.concatenate([wave[:length], wave[length:]], 1) for wave in middle]
    result = [
        jnp.dot(wave, right_table, preferred_element_type=jnp.float32) for wave in middle
    ]
    return [(wave[:, :length], wave[:, length:]) for wave in result]


def transforms(waves, left_table, right_table):
    stacked = [
        jnp.concatenate([part.astype(jnp.bfloat16) for part in wave], 0) for wave in waves
    ]
    return sections(stacked, left_table, right_table)


def product_of(left, right):
    return left[0] * right[0] - left[1] * right[1], left[0] * right[1] + left[1] * right[0]


def conj_product(left, right):
    return left[0] * right[0] + left[1] * right[1], left[1] * right[0] - left[0] * right[1]


def strip_copies(array, strips, row0, store, plane, sem, outward):
    copies = []
    for s in range(array.shape[0]):
        for c in range(array.shape[1]):
            for k, strip in enumerate(strips):
                whole = array.at[s, c, :, pl.ds(k * lanes, lanes)]
                part = store.at[plane + s, c, strip, pl.ds(row0, array.shape[2]), :]
                source, target = (part, whole) if outward else (whole, part)
                copies.append(pltpu.make_async_copy(source, target, sem))
    return copies


def run_copies(groups):
    copies = [copy for group in groups for copy in group]
    for copy in copies:
        copy.start()
    return copies


def finish(copies):
    for copy in copies:
        copy.wait()


def patch_spot(places, slot):
    column = places[2 * slot + 1]
    return places[2 * slot], column // lanes, lax.rem(column, lanes)


def fetch(window, s, spot, length):
    row, strip, shift = spot
    back = lax.rem(lanes - shift, lanes)
    lane = lax.broadcasted_iota(jnp.int32, (length, lanes), 1)
    out = []
    for c in range(2):
        rolled = [
            pltpu.roll(window[s, c, strip + k, pl.ds(row, length), :], back, 1)
            for k in range(length // lanes + 1)
        ]
        parts = [
            jnp.where(lane < lanes - shift, rolled[k], rolled[k + 1])
            for k in range(length // lanes)
        ]
        out.append(jnp.concatenate(parts, 1))
    return tuple(out)


def accumulate(gradient, s, spot, wave, length):
    row, strip, shift = spot
    lane = lax.broadcasted_iota(jnp.int32, (length, lanes), 1)
    count = length // lanes
    for c in range(2):
        rolled = [
            pltpu.roll(wave[c][:, k * lanes : (k + 1) * lanes], shift, 1) for k in range(count)
        ]
        for k in range(count + 1):
            if k == 0:
                part = jnp.where(lane >= shift, rolled[0], 0.0)
            elif k == count:
                part = jnp.where(lane < shift, rolled[k - 1], 0.0)
            else:
                part = jnp.where(lane < shift, rolled[k - 1], rolled[k])
            at = (s, c, strip + k, pl.ds(row, length), slice(None))
            gradient[at] = gradient[at] + part


def spread_slots(places, window, constants, spreads, slots):
    probe, propagator, _, table_a, table_b = constants
    length = probe.shape[-1]
    waves = [
        product_of((probe[0], probe[1]), fetch(window, 0, patch_spot(places, slot), length))
        for slot in slots
    ]
    waves = transforms(waves, table_a[...], table_b[...])
    waves = [product_of((propagator[0], propagator[1]), wave) for wave in waves]
    waves = transforms(waves, table_b[...], table_a[...])
    for wave, slot in zip(waves, slots):
        spreads[slot, 0] = wave[0]
        spreads[slot, 1] = wave[1]


def back_slots(places, window, gradient, constants, spreads, inners, slots):
    probe, _, measured_ref, table_a, table_b = constants
    length = probe.shape[-1]
    spots = [patch_spot(places, slot) for slot in slots]
    waves = [
        product_of((spreads[slot, 0], spreads[slot, 1]), fetch(window, 1, spot, length))
        for slot, spot in zip(slots, spots)
    ]
    residuals = []
    for far, slot in zip(transforms(waves, table_a[...], table_b[...]), slots):
        power = far[0] * far[0] + far[1] * far[1]
        measured = measured_ref[slot].astype(jnp.float32)
        ratio = 1.0 - measured * jnp.minimum(lax.rsqrt(power), 1.0 / floor_value)
        residuals.append((far[0] * ratio, far[1] * ratio))
    backs = transforms(residuals, table_b[...], table_a[...])
    for back, slot, spot in zip(backs, slots, spots):
        inner = conj_product(back, fetch(window, 1, spot, length))
        inners[slot, pl.ds(0, length), :] = inner[0].astype(jnp.bfloat16)
        inners[slot, pl.ds(length, length), :] = inner[1].astype(jnp.bfloat16)
        spread = (spreads[slot, 0], spreads[slot, 1])
        accumulate(gradient, 1, spot, conj_product(back, spread), length)


def first_slots(places, gradient, constants, inners, slots):
    probe, propagator, _, table_a, table_b = constants
    length = probe.shape[-1]
    waves = sections([inners[slot] for slot in slots], table_a[...], table_b[...])
    waves = [conj_product(wave, (propagator[0], propagator[1])) for wave in waves]
    waves = transforms(waves, table_b[...], table_a[...])
    for wave, slot in zip(waves, slots):
        grad = conj_product(wave, (probe[0], probe[1]))
        accumulate(gradient, 0, patch_spot(places, slot), grad, length)


def visit_slots(places, count, slots, wanted, todo, threes, visit):
    def pick(slot, found):
        chosen = jnp.logical_and(
            slot < count[0], wanted(places[2 * slot], places[2 * slot + 1])
        )

        @pl.when(chosen)
        def _():
            todo[found] = slot

        return found + chosen.astype(jnp.int32)

    found = lax.fori_loop(0, slots, pick, jnp.int32(0))
    odd = lax.rem(found, 2) == 1
    three = jnp.logical_and(odd, found >= 3) if threes else jnp.bool_(False)

    def pair(index, carry):
        visit([todo[2 * index], todo[2 * index + 1]])
        return carry

    lax.fori_loop(0, (found - 3 * three.astype(jnp.int32)) // 2, pair, 0)
    if threes:

        @pl.when(three)
        def _():
            visit([todo[found - 3], todo[found - 2], todo[found - 1]])

    @pl.when(jnp.logical_and(odd, jnp.logical_not(three)))
    def _():
        visit([todo[found - 1]])


def slot_groups(tile, length, split):
    limit = tile - length

    def inside(row, column):
        return jnp.logical_and(row <= limit, column <= limit)

    def outside(row, column):
        return jnp.logical_not(inside(row, column))

    def upper(row, column):
        return jnp.logical_and(outside(row, column), row <= limit + split)

    def lower(row, column):
        return row > limit + split

    return inside, outside, upper, lower


def sizes(tile, length):
    own = range(tile // lanes)
    near = range(length // lanes)
    far = range(length // lanes, tile // lanes)
    past = range(tile // lanes, (tile + length) // lanes)
    return own, near, far, past


def from_strips(out, strips, row0, store, plane):
    for s in range(out.shape[0]):
        for c in range(out.shape[1]):
            for k, strip in enumerate(strips):
                out[s, c, :, pl.ds(k * lanes, lanes)] = store[
                    plane + s, c, strip, pl.ds(row0, out.shape[2]), :
                ]


def into_strips(piece, strips, row0, store, plane):
    for c in range(piece.shape[1]):
        for k, strip in enumerate(strips):
            store[plane, c, strip, pl.ds(row0, piece.shape[2]), :] = piece[
                0, c, :, pl.ds(k * lanes, lanes)
            ]


def pack_near_kernel(object_ref, start, out, sem):
    del start
    finish(run_copies([corner_copies(object_ref, out, sem, False)]))


def pack_kernel(corners, object_ref, *rest):
    outs, sem = rest[:-1], rest[-1]
    copies = []
    for (s, row, column), out in zip(corners, outs):
        for c in range(out.shape[1]):
            piece = object_ref.at[
                s, c, pl.ds(row, out.shape[2]), pl.ds(column, out.shape[3])
            ]
            copies.append(pltpu.make_async_copy(piece, out.at[0, c], sem))
    for copy in copies:
        copy.start()
    finish(copies)


def pack(object_field, pieces):
    return pl.pallas_call(
        functools.partial(pack_kernel, [piece[:3] for piece in pieces]),
        out_shape=[
            pltpu.VMEM((1, object_field.shape[1], *piece[3:]), jnp.float32)
            for piece in pieces
        ],
        in_specs=[hbm_space],
        out_specs=[vmem_space] * len(pieces),
        scratch_shapes=[pltpu.SemaphoreType.DMA],
        compiler_params=pltpu.CompilerParams(vmem_limit_bytes=6 * 1024 * 1024),
    )(in_hbm(object_field))


def own_slots_kernel(places, count, object_ref, *rest):
    constants, (window, gradient, spreads, inners, todo, sem) = rest[:5], rest[5:]
    length = constants[0].shape[-1]
    tile = object_ref.shape[-1]
    own, _, _, _ = sizes(tile, length)
    loads = run_copies([strip_copies(object_ref, own, 0, window, 0, sem, False)])
    gradient[...] = jnp.zeros_like(gradient)
    finish(loads)

    def visit(slots):
        spread_slots(places, window, constants, spreads, slots)
        back_slots(places, window, gradient, constants, spreads, inners, slots)

    inside, _, _, _ = slot_groups(tile, length, length // 2)
    visit_slots(places, count, inners.shape[0], inside, todo, False, visit)


def spread_kernel(places, count, near_ref, far_ref, corner_ref, right_ref, *rest):
    constants, (window, gradient, spreads, inners, todo, sem) = rest[:5], rest[9:]
    length = constants[0].shape[-1]
    tile = right_ref.shape[2]
    _, near, far, past = sizes(tile, length)
    finish(
        run_copies(
            [
                strip_copies(near_ref, near, tile, window, 0, sem, False),
                strip_copies(far_ref, far, tile, window, 0, sem, False),
                strip_copies(corner_ref, past, tile, window, 0, sem, False),
                strip_copies(right_ref, past, 0, window, 0, sem, False),
            ]
        )
    )

    def visit(slots):
        spread_slots(places, window, constants, spreads, slots)

    _, outside, _, _ = slot_groups(tile, length, length // 2)
    visit_slots(places, count, inners.shape[0], outside, todo, False, visit)


def upper_kernel(places, count, near_ref, corner_ref, right_ref, far_ref, *rest):
    constants, (window, gradient, spreads, inners, todo, sem) = rest[:5], rest[9:]
    length = constants[0].shape[-1]
    tile = right_ref.shape[2]
    split = far_ref.shape[2]
    _, near, far, past = sizes(tile, length)
    finish(
        run_copies(
            [
                strip_copies(near_ref, near, tile, window, 1, sem, False),
                strip_copies(corner_ref, past, tile, window, 1, sem, False),
                strip_copies(right_ref, past, 0, window, 1, sem, False),
                strip_copies(far_ref, far, tile, window, 1, sem, False),
            ]
        )
    )

    def visit(slots):
        back_slots(places, window, gradient, constants, spreads, inners, slots)

    _, _, upper, _ = slot_groups(tile, length, split)
    visit_slots(places, count, inners.shape[0], upper, todo, False, visit)


def back_kernel(places, count, far_ref, *rest):
    constants = rest[:5]
    near_out, far_out, corner_out, window, gradient, spreads, inners, todo, _ = rest[9:]
    length = constants[0].shape[-1]
    tile = length + far_ref.shape[3]
    _, near, far, past = sizes(tile, length)
    split = length - far_ref.shape[2]
    into_strips(far_ref, far, tile + split, window, 1)

    def visit(slots):
        back_slots(places, window, gradient, constants, spreads, inners, slots)

    _, _, _, lower = slot_groups(tile, length, split)
    visit_slots(places, count, inners.shape[0], lower, todo, True, visit)
    from_strips(corner_out, past, tile, gradient, 1)
    from_strips(far_out, far, tile, gradient, 1)
    from_strips(near_out, near, tile, gradient, 1)


def first_kernel(places, count, *rest):
    constants = rest[:5]
    near_out, far_out, corner_out, right_out = rest[9:13]
    _, gradient, _, inners, todo, _ = rest[13:]
    length = constants[0].shape[-1]
    tile = length + far_out.shape[3]
    _, near, far, past = sizes(tile, length)

    def visit(slots):
        first_slots(places, gradient, constants, inners, slots)

    def all_slots(row, column):
        return row >= 0

    visit_slots(places, count, inners.shape[0], all_slots, todo, False, visit)
    from_strips(corner_out, past, tile, gradient, 0)
    from_strips(far_out, far, tile, gradient, 0)
    from_strips(near_out, near, tile, gradient, 0)
    from_strips(right_out, past, 0, gradient, 0)


def own_kernel(gradient, own_out, sem):
    tile = own_out.shape[-1]
    finish(run_copies([strip_copies(own_out, range(tile // lanes), 0, gradient, 0, sem, True)]))


def add_kernel(plane, column, gradient_in, piece_ref, gradient_out, held, added, sems):
    del gradient_in
    slices, parts, rows, columns = piece_ref.shape
    planes = [(s, c) for s in range(slices) for c in range(parts)]

    def spot(s, c):
        return gradient_out.at[plane + s, c, pl.ds(0, rows), pl.ds(column, columns)]

    loads, pieces, stores = [], [], []
    for i, (s, c) in enumerate(planes):
        loads.append(pltpu.make_async_copy(spot(s, c), held.at[i], sems.at[0, i]))
        pieces.append(pltpu.make_async_copy(piece_ref.at[s, c], added.at[i], sems.at[1, i]))
        stores.append(pltpu.make_async_copy(held.at[i], spot(s, c), sems.at[2, i]))
        loads[i].start()
        pieces[i].start()
    for i in range(len(planes)):
        loads[i].wait()
        pieces[i].wait()
        held[i] = held[i] + added[i]
        stores[i].start()
    finish(stores)


def add_piece(gradient, piece, plane, column):
    slices, parts, rows, columns = piece.shape
    planes = slices * parts
    return pl.pallas_call(
        functools.partial(add_kernel, plane, column),
        out_shape=jax.ShapeDtypeStruct(gradient.shape, gradient.dtype),
        in_specs=[any_space] * 2,
        out_specs=any_space,
        scratch_shapes=[pltpu.VMEM((planes, rows, columns), jnp.float32)] * 2
        + [pltpu.SemaphoreType.DMA((3, planes))],
        input_output_aliases={0: 0},
        compiler_params=pltpu.CompilerParams(vmem_limit_bytes=8 * 1024 * 1024),
    )(gradient, piece)


def corner_copies(gradient, held, sem, outward):
    copies = []
    for c in range(held.shape[1]):
        part = gradient.at[0, c, pl.ds(0, held.shape[2]), pl.ds(0, held.shape[3])]
        source, target = (held.at[0, c], part) if outward else (part, held.at[0, c])
        copies.append(pltpu.make_async_copy(source, target, sem))
    return copies


def hold_kernel(gradient, held, sem):
    finish(run_copies([corner_copies(gradient, held, sem, False)]))


def last_kernel(gradient_in, held, piece, gradient, total, sem):
    del gradient_in
    stores = corner_copies(gradient, total, sem, True)
    for c, store in enumerate(stores):
        total[0, c] = held[0, c] + piece[0, c]
        store.start()
    finish(stores)


def in_hbm(x):
    return pltpu.with_memory_space_constraint(x, pltpu.HBM)


def in_vmem(x):
    return pltpu.with_memory_space_constraint(x, pltpu.VMEM)


any_space = pl.BlockSpec(memory_space=pl.ANY)
hbm_space = pl.BlockSpec(memory_space=pltpu.HBM)
vmem_space = pl.BlockSpec(memory_space=pltpu.VMEM)
scalar_space = pl.BlockSpec(memory_space=pltpu.SMEM)


def slots_call(body, scalars, pieces, constants, state, state_types, out_shapes):
    first = len(scalars) + len(pieces) + len(constants)
    aliases = {first + i: len(out_shapes) + i for i in range(len(state))}
    close = bool(out_shapes)
    if close:
        pieces = [in_vmem(piece) for piece in pieces]
    piece_space = vmem_space if close else any_space if state else hbm_space
    return pl.pallas_call(
        body,
        out_shape=[pltpu.VMEM(s, jnp.float32) for s in out_shapes] + state_types,
        in_specs=[scalar_space] * len(scalars)
        + [piece_space] * len(pieces)
        + [vmem_space] * (len(constants) + len(state)),
        out_specs=[vmem_space] * (len(out_shapes) + len(state_types)),
        scratch_shapes=[
            pltpu.SMEM((constants[2].shape[0],), jnp.int32),
            pltpu.SemaphoreType.DMA,
        ],
        input_output_aliases=aliases,
        compiler_params=pltpu.CompilerParams(vmem_limit_bytes=20 * 1024 * 1024),
    )(*scalars, *pieces, *[in_vmem(x) for x in (*constants, *state)])


def tile_gradient(object_field, probe_field, propagator_phase, positions, counts, amplitudes):
    length = probe_field.shape[-1]
    tile = object_field.shape[-1]
    slices, parts = object_field.shape[:2]
    slots = positions.shape[-2]

    rest = tile - length
    near0 = pl.pallas_call(
        pack_near_kernel,
        name="pack0",
        out_shape=pltpu.VMEM((1, parts, length, length), jnp.float32),
        in_specs=[hbm_space, vmem_space],
        out_specs=vmem_space,
        scratch_shapes=[pltpu.SemaphoreType.DMA],
        input_output_aliases={1: 0},
        compiler_params=pltpu.CompilerParams(vmem_limit_bytes=1024 * 1024),
    )(in_hbm(object_field), in_vmem(jnp.zeros((1, parts, length, length), jnp.float32)))
    split = length // 2
    right0, near1, far0, upper1, lower1, right1 = pack(
        object_field,
        [
            (0, 0, 0, tile, length),
            (1, 0, 0, length, length),
            (0, 0, length, length, rest),
            (1, 0, length, split, rest),
            (1, split, length, length - split, rest),
            (1, 0, 0, tile, length),
        ],
    )
    near0 = shifted(near0, "row", -1)
    right0 = shifted(right0, "col", -1)
    near1 = shifted(near1, "row", -1)
    far0 = shifted(far0, "row", -1)
    upper1 = shifted(upper1, "row", -1)
    lower1 = shifted(lower1, "row", -1)
    right1 = shifted(right1, "col", -1)
    corner0 = shifted(near0, "col", -1)
    corner1 = shifted(near1, "col", -1)

    propagator = jnp.stack([jnp.cos(propagator_phase), jnp.sin(propagator_phase)], 0)
    constants = (probe_field, propagator, amplitudes[0, 0], *dft_tables(length))
    scalars = (positions.reshape(-1), counts.reshape(-1))
    strips = (slices, parts, (tile + length) // lanes, tile + length, lanes)
    state_types = [
        pltpu.VMEM(strips, jnp.float32),
        pltpu.VMEM(strips, jnp.float32),
        pltpu.VMEM((slots, parts, length, length), jnp.float32),
        pltpu.VMEM((slots, parts * length, length), jnp.bfloat16),
    ]
    piece_shapes = (
        (1, parts, length, length),
        (1, parts, length, tile - length),
        (1, parts, length, length),
    )

    def call(kernel, pieces, state, out_shapes):
        return slots_call(kernel, scalars, pieces, constants, state, state_types, out_shapes)

    state = call(own_slots_kernel, (in_hbm(object_field),), (), ())
    state = call(spread_kernel, (near0, far0, corner0, right0), state, ())
    state = call(upper_kernel, (near1, corner1, right1, upper1), state, ())
    near1, far1, corner1, *state = call(back_kernel, (lower1,), state, piece_shapes)
    corner1 = shifted(corner1, "col", 1)
    far1 = shifted(far1, "row", 1)
    near0, far0, corner0, right, window, gradient, *_ = call(
        first_kernel, (), state, (*piece_shapes, (slices, parts, tile, length))
    )
    near1 = shifted(near1 + corner1, "row", 1)
    corner0 = shifted(corner0, "col", 1)
    right = shifted(right, "col", 1)
    far0 = shifted(far0, "row", 1)
    own = pl.pallas_call(
        own_kernel,
        name="store",
        out_shape=jax.ShapeDtypeStruct(object_field.shape, jnp.float32),
        in_specs=[vmem_space],
        out_specs=any_space,
        scratch_shapes=[pltpu.SemaphoreType.DMA],
        compiler_params=pltpu.CompilerParams(vmem_limit_bytes=1024 * 1024),
    )(in_vmem(gradient))
    near0 = shifted(near0 + corner0, "row", 1)
    result = add_piece(own, far1, 1, length)
    result = add_piece(result, near1, 1, 0)
    result = add_piece(result, right, 0, 0)
    result = add_piece(result, far0, 0, length)
    held = pl.pallas_call(
        hold_kernel,
        name="hold",
        out_shape=pltpu.VMEM(near0.shape, jnp.float32),
        in_specs=[any_space],
        out_specs=vmem_space,
        scratch_shapes=[pltpu.SemaphoreType.DMA],
        compiler_params=pltpu.CompilerParams(vmem_limit_bytes=2 * 1024 * 1024),
    )(in_hbm(result))
    return pl.pallas_call(
        last_kernel,
        name="addn0",
        out_shape=jax.ShapeDtypeStruct(result.shape, jnp.float32),
        in_specs=[any_space, vmem_space, vmem_space],
        out_specs=any_space,
        scratch_shapes=[pltpu.VMEM(near0.shape, jnp.float32), pltpu.SemaphoreType.DMA],
        input_output_aliases={0: 0},
        compiler_params=pltpu.CompilerParams(vmem_limit_bytes=2 * 1024 * 1024),
    )(result, in_vmem(held), in_vmem(near0))


def solution(mesh):
    return jax.shard_map(
        tile_gradient,
        mesh=mesh,
        in_specs=(
            P(None, None, "row", "col"),
            P(),
            P(),
            P("row", "col", None, None),
            P("row", "col"),
            P("row", "col", None, None, None),
        ),
        out_specs=P(None, None, "row", "col"),
        check_vma=False,
    )
```
